32 devices in a mesh: rows: 32 (over z, y, x, core).
Axes of the slice: x: 2, y: 2, z: 4, core: 2. Of those that a mesh axis runs over, the one named last changes fastest.
Arguments:
- stiffness: float32 [9, 128, 512], P(None, 'rows'), may hold values from -400 to 806.1, as said below
- mass: float32 [9, 128, 512], P(None, 'rows'), may hold values from 0.05 to 3, as said below
- shifts: float32 [3], replicated, may hold values from 0.05 to 2
- factor: float32 [128, 32, 512], P('rows'), may hold values from -6 to 6
Outputs:
- lowrank: float32 [3, 128, 32, 512], P(None, 'rows')
- residual_factor: float32 [128, 32, 512], P('rows')
The draws below stay inside these ranges and needn't reach their ends.
Inputs may be any that keep to these rules, and one draw needn't show every extreme that they name: `stiffness`: entry 4 along the first dimension exceeds the sum of the magnitudes of the other eight, which are negative. `mass`: entry 4 along the first dimension exceeds the sum of the other eight, which are positive.
All inputs are finite; a program needn't handle non-finite values.
Results may differ from the reference program's by a relative error of at most 0.0003.
Values sent between devices are 32-bit elements; how exact they have to be, the bound alone decides.
No kernel may reach another device: no remote copies, remote signals or barrier semaphores. Data moves between devices by JAX's collectives and lax.ppermute only.
A program may use at most 128 MiB of HBM per device.

```python
import math
import jax
import jax.numpy as jnp
from jax import lax

NC = 512
NRHS = 32
STEPS = 3
ITERS = 4
NR = 128


def draw_stiffness(key, part):
    key = jax.random.fold_in(key, 11)
    first, second, third = jax.random.split(key, 3)
    others = -(0.2 + 0.8 * jax.random.uniform(first, (6, NR, NC), jnp.float32))
    along = -(100.0 + 300.0 * jax.random.uniform(third, (2, NR, NC), jnp.float32))
    extra = 0.02 + 0.08 * jax.random.uniform(second, (1, NR, NC), jnp.float32)
    center = -jnp.sum(others, axis=0, keepdims=True) - jnp.sum(along, axis=0, keepdims=True) + extra
    return jnp.concatenate([others[:3], along[:1], center, along[1:], others[3:]], axis=0)


def draw_mass(key, part):
    key = jax.random.fold_in(key, 23)
    first, second = jax.random.split(key)
    offdiag = 0.05 + 0.2 * jax.random.uniform(first, (8, NR, NC), jnp.float32)
    extra = 0.2 + 0.8 * jax.random.uniform(second, (1, NR, NC), jnp.float32)
    center = jnp.sum(offdiag, axis=0, keepdims=True) + extra
    return jnp.concatenate([offdiag[:4], center, offdiag[4:]], axis=0)


def level_of(own_key, dims, cuts, smallest, top_value):
    level = 1.0
    for axis_at, parts in cuts:
        draws = jax.random.uniform(jax.random.fold_in(jax.random.fold_in(own_key, 6), axis_at), (parts,), jnp.float32, smallest / len(cuts), top_value / len(cuts))
        level = level * jnp.repeat(jnp.exp(draws), dims[axis_at] // parts).reshape((-1,) + (1,) * (len(dims) - 1 - axis_at))
    return level


def noise(own_key, shape, width, bound, cuts=(), kind=jnp.bfloat16):
    array = width * jax.random.normal(own_key, shape, jnp.float32)
    if cuts:
        array = array * level_of(own_key, shape, cuts, -0.22, 0.18)
    return jnp.clip(array, -bound, bound).astype(kind)


def setup_inputs(seed: int = 0) -> dict:
    splits = jax.random.split(jax.random.key(seed), 5)
    return {
        "stiffness": draw_stiffness(jax.random.fold_in(splits[4], 71), 0),
        "mass": draw_mass(jax.random.fold_in(splits[4], 71), 0),
        "shifts": jnp.clip(jnp.exp(jax.random.uniform(splits[2], (STEPS,), jnp.float32, math.log(0.05), math.log(2.0))), 0.05, 2.0),
        "factor": noise(splits[3], (NR, NRHS, NC), 1.0, 6.0, ((0, 32),), jnp.float32),
    }


OFFSETS = ((-1, -1), (-1, 0), (-1, 1), (0, -1), (0, 0), (0, 1), (1, -1), (1, 0), (1, 1))

def apply_stencil(coeffs, padded):
    height = coeffs.shape[1]
    breadth = padded.shape[2]
    framed = jnp.pad(padded, ((0, 0), (0, 0), (1, 1)))
    summed = jnp.zeros((height, padded.shape[1], breadth), padded.dtype)
    for stencil_entry, offset in enumerate(OFFSETS):
        shifted = framed[1 + offset[0]:1 + offset[0] + height, :, 1 + offset[1]:1 + offset[1] + breadth]
        summed = summed + coeffs[stencil_entry][:, None, :] * shifted
    return summed

def line_solve(coeffs, vector):
    breadth = vector.shape[2]
    column = lax.broadcasted_iota(jnp.int32, (1, breadth), 1)
    below_diag = jnp.where(column == 0, 0.0, coeffs[3]).astype(vector.dtype)
    above_diag = jnp.where(column == breadth - 1, 0.0, coeffs[5]).astype(vector.dtype)
    extent = vector.shape
    below_diag = jnp.broadcast_to(below_diag[:, None, :], extent)
    center = jnp.broadcast_to(coeffs[4][:, None, :], extent)
    above_diag = jnp.broadcast_to(above_diag[:, None, :], extent)
    solved = lax.linalg.tridiagonal_solve(below_diag, center, above_diag, vector[..., None])
    return solved[..., 0]

def pad_rows(field):
    return jnp.pad(field, ((1, 1), (0, 0), (0, 0)))

def row_sums(field):
    return lax.optimization_barrier(jnp.sum(field, axis=(0, 2)))

def least_squares(columns, initial):
    count = len(columns)
    cosines = []
    sines = []
    rhs_list = [initial] + [jnp.zeros_like(initial) for onward in range(count)]
    upper_cols = []
    for position in range(count):
        column = list(columns[position])
        for earlier in range(position):
            first = cosines[earlier] * column[earlier] + sines[earlier] * column[earlier + 1]
            second = -sines[earlier] * column[earlier] + cosines[earlier] * column[earlier + 1]
            column[earlier] = first
            column[earlier + 1] = second
        radius = jnp.sqrt(column[position] * column[position] + column[position + 1] * column[position + 1])
        cosine = column[position] / radius
        sine = column[position + 1] / radius
        cosines.append(cosine)
        sines.append(sine)
        column[position] = radius
        rhs_list[position + 1] = -sine * rhs_list[position]
        rhs_list[position] = cosine * rhs_list[position]
        upper_cols.append(column[:position + 1])
    solution = [None] * count
    for position in reversed(range(count)):
        accum = rhs_list[position]
        for onward in range(position + 1, count):
            accum = accum - upper_cols[onward][position] * solution[onward]
        solution[position] = accum / upper_cols[position][position]
    return solution

def shifted_solve(coeffs, right_side):
    initial = jnp.sqrt(row_sums(right_side * right_side))
    krylov = [right_side / initial[None, :, None]]
    directions = []
    columns = []
    for krylov_step in range(ITERS):
        direction = line_solve(coeffs, krylov[krylov_step])
        directions.append(direction)
        mapped = apply_stencil(coeffs, pad_rows(direction))
        heights = jnp.stack([row_sums(vector * mapped) for vector in krylov])
        for earlier in range(krylov_step + 1):
            mapped = mapped - heights[earlier][None, :, None] * krylov[earlier]
        remainder = jnp.sqrt(row_sums(mapped * mapped))
        columns.append([heights[earlier] for earlier in range(krylov_step + 1)] + [remainder])
        if krylov_step + 1 < ITERS:
            krylov.append(mapped / remainder[None, :, None])
    weights = least_squares(columns, initial)
    result = weights[0][None, :, None] * directions[0]
    for onward in range(1, ITERS):
        result = result + weights[onward][None, :, None] * directions[onward]
    return result

def reference(stiffness, mass, shifts, factor):
    current = factor
    pieces = []
    for adi_step in range(STEPS):
        shift_now = shifts[adi_step]
        coeffs = stiffness + shift_now * mass
        result = shifted_solve(coeffs, current)
        pieces.append(jnp.sqrt(2.0 * shift_now) * result)
        current = current - 2.0 * shift_now * apply_stencil(mass, pad_rows(result))
    return (jnp.stack(pieces), current)
```

```python
import functools

import jax
import jax.numpy as jnp
from jax import lax
from jax.experimental import pallas as pl
from jax.experimental.pallas import tpu as pltpu
from jax.sharding import PartitionSpec as P

ITERS = 4
CELLS = 4
LANES = 128
PIVOT_TOL = 3e-7
OFFSETS = ((-1, -1), (-1, 0), (-1, 1), (0, -1), (0, 0), (0, 1), (1, -1), (1, 0), (1, 1))
OFF_ROW = (0, 1, 2, 6, 7, 8)
PAIRS = [(i, j) for i in range(ITERS + 1) for j in range(i, ITERS + 1)]


E1, E2, G0, G1, G2, C0, C1, A3, C3, L0, L1, L2, R0, R1, R2, INV = range(16)
LEVELS = 16


def roll(x, shift, axis=-1):
    axis = axis % x.ndim
    return pltpu.roll(x, shift % x.shape[axis], axis)


def params():
    return pltpu.CompilerParams(vmem_limit_bytes=40 * 1024 * 1024)


def to_chunks(natural, stage):
    tiles = natural.shape[1] // LANES
    for tile in range(tiles):
        stage[tile * LANES : (tile + 1) * LANES, :] = natural[:, tile * LANES : (tile + 1) * LANES].T
    return [stage[pl.ds(cell, LANES, stride=CELLS), :].T for cell in range(CELLS)]


def from_chunks(planes, stage):
    for cell in range(CELLS):
        stage[pl.ds(cell, LANES, stride=CELLS), :] = planes[cell].T
    return [stage[tile * LANES : (tile + 1) * LANES, :].T for tile in range(CELLS)]


def pack_kernel(stiff_ref, mass_ref, factor_ref, out_ref, stage, gather):
    rows, cols, width = factor_ref.shape
    planes = to_chunks(factor_ref[...].reshape(rows * cols, width), stage)
    for cell in range(CELLS):
        out_ref[cell, 0 : rows * cols, :] = planes[cell]
    entries = len(OFFSETS)
    gather[...] = jnp.zeros(gather.shape, jnp.float32)
    for which, ref in enumerate((stiff_ref, mass_ref)):
        for entry in range(entries):
            at = (which * entries + entry) * rows
            gather[at : at + rows, :] = ref[entry]
    planes = to_chunks(gather[...], stage)
    count = 2 * entries * rows
    lane = lax.broadcasted_iota(jnp.int32, (count, LANES), 1)
    line = lax.broadcasted_iota(jnp.int32, (count, LANES), 0)
    column = (line // rows) % 3
    for cell in range(CELLS):
        plane = planes[cell][0:count, :]
        if cell == 0:
            plane = jnp.where((lane == 0) & (column == 0), 0.0, plane)
        if cell == CELLS - 1:
            plane = jnp.where((lane == LANES - 1) & (column == 2), 0.0, plane)
        out_ref[cell, rows * cols : rows * cols + count, :] = plane


def build_line_factors(diag, factors, rows_ext):
    def put(index, value):
        factors[index, 0:rows_ext, :] = value

    a = [diag(3, cell) for cell in range(CELLS)]
    d = [diag(4, cell) for cell in range(CELLS)]
    c = [diag(5, cell) for cell in range(CELLS)]
    d = [jnp.where(x <= 0.0, 1.0, x) for x in d]
    g0 = 1.0 / d[0]
    e1 = a[1] * g0
    g1 = 1.0 / (d[1] - e1 * c[0])
    e2 = a[2] * g1
    g2 = 1.0 / (d[2] - e2 * c[1])
    f0 = -a[0]
    f1 = -e1 * f0
    f2 = -e2 * f1
    l2 = f2 * g2
    l1 = (f1 - c[1] * l2) * g1
    l0 = (f0 - c[0] * l1) * g0
    r2 = -c[2] * g2
    r1 = -c[1] * r2 * g1
    r0 = -c[0] * r1 * g0
    below = a[3] * l2
    center = d[3] + a[3] * r2 + c[3] * roll(l0, -1)
    above = c[3] * roll(r0, -1)
    for index, value in (
        (E1, e1), (E2, e2), (G0, g0), (G1, g1), (G2, g2), (C0, c[0]), (C1, c[1]), (A3, a[3]),
        (C3, c[3]), (L0, l0), (L1, l1), (L2, l2), (R0, r0), (R1, r1), (R2, r2),
    ):
        put(index, value)
    stride = 1
    slot = LEVELS
    while stride < LANES:
        inverse = 1.0 / center
        from_below = -below * roll(inverse, stride)
        from_above = -above * roll(inverse, -stride)
        center = center + from_below * roll(above, stride) + from_above * roll(below, -stride)
        below = from_below * roll(below, stride)
        above = from_above * roll(above, -stride)
        put(slot, from_below)
        put(slot + 1, from_above)
        slot += 2
        stride *= 2
    put(INV, 1.0 / center)


def level_count():
    return LANES.bit_length() - 1


def line_solve(factors, read, rows, cols, write):
    def coef(index, row):
        return factors[index, row : row + 1, :]

    p0, p1, p2, s = [], [], [], []
    for row in rows:
        v0, v1, v2, v3 = (read(cell, row) for cell in range(CELLS))
        f1 = v1 - coef(E1, row) * v0
        f2 = v2 - coef(E2, row) * f1
        x2 = f2 * coef(G2, row)
        x1 = (f1 - coef(C1, row) * x2) * coef(G1, row)
        x0 = (v0 - coef(C0, row) * x1) * coef(G0, row)
        p0.append(x0)
        p1.append(x1)
        p2.append(x2)
        s.append(v3 - coef(A3, row) * x2 - coef(C3, row) * roll(x0, -1))
    stride = 1
    slot = LEVELS
    while stride < LANES:
        for at, row in enumerate(rows):
            if 2 * stride == LANES:
                both = coef(slot, row) + coef(slot + 1, row)
                s[at] = s[at] + both * roll(s[at], stride)
            else:
                s[at] = (
                    s[at]
                    + coef(slot, row) * roll(s[at], stride)
                    + coef(slot + 1, row) * roll(s[at], -stride)
                )
        slot += 2
        stride *= 2
    for at, row in enumerate(rows):
        x3 = s[at] * coef(INV, row)
        before = roll(x3, 1)
        x0 = p0[at] + coef(L0, row) * before + coef(R0, row) * x3
        x1 = p1[at] + coef(L1, row) * before + coef(R1, row) * x3
        x2 = p2[at] + coef(L2, row) * before + coef(R2, row) * x3
        write(row, (before, x0, x1, x2, x3, roll(x0, -1)))


def stencil_rows(coef, entries, read, row):
    out = []
    for cell in range(CELLS):
        total = None
        for entry in entries:
            offset = OFFSETS[entry]
            term = coef(entry, cell) * read(1 + cell + offset[1], row + offset[0])
            total = term if total is None else total + term
        out.append(total)
    return out


def krylov_kernel(
    parity_ref, shift_ref, mine_ref, even_ref, odd_ref, coefs_in, *refs, step, first, rows, cols, peers
):
    if first:
        coefs_ref, z_out, gram_out, wx, zx, line, factors = refs
    else:
        z_out, gram_out, wx, zx, line, factors = refs
        coefs_ref = coefs_in
    ext = 3 * rows
    entries = len(OFFSETS)
    block = rows * cols
    parity = parity_ref[0]
    at_even = jnp.where(parity == 0, 2 * rows, 0)
    at_odd = 2 * rows - at_even
    wx[0, :, pl.ds(rows * cols, block), :] = mine_ref[:, 0:block, :]
    wx[0, :, pl.ds(pl.multiple_of(at_even * cols, cols), block), :] = even_ref[:, 0:block, :]
    wx[0, :, pl.ds(pl.multiple_of(at_odd * cols, cols), block), :] = odd_ref[:, 0:block, :]
    if first:
        low_is_even = parity == 1
        for which in range(2):
            for entry in range(entries):
                at = block + (which * entries + entry) * rows
                for cell in range(CELLS):
                    even = even_ref[cell, at : at + rows, :]
                    odd = odd_ref[cell, at : at + rows, :]
                    coefs_ref[which, entry, cell, 0:rows, :] = jnp.where(low_is_even, even, odd)
                    coefs_ref[which, entry, cell, rows : 2 * rows, :] = mine_ref[cell, at : at + rows, :]
                    coefs_ref[which, entry, cell, 2 * rows : ext, :] = jnp.where(low_is_even, odd, even)
    shift = shift_ref[step]
    for entry in range(entries):
        for cell in range(CELLS):
            line[entry, cell, 0:ext, :] = (
                coefs_ref[0, entry, cell, 0:ext, :] + shift * coefs_ref[1, entry, cell, 0:ext, :]
            )
    build_line_factors(lambda entry, cell: line[entry, cell, 0:ext, :], factors, ext)

    for k in range(ITERS):
        low, high = k, ext - k

        def read_w(cell, row):
            return wx[k, cell, row * cols : (row + 1) * cols, :]

        def write_z(row, slots):
            for slot, value in enumerate(slots):
                zx[slot, row * cols : (row + 1) * cols, :] = value
            if rows - 1 <= row <= 2 * rows:
                at = (row - rows + 1) * cols
                for cell in range(CELLS):
                    z_out[k, cell, at : at + cols, :] = slots[1 + cell]

        for row in range(low, high, 2):
            line_solve(factors, read_w, list(range(row, min(row + 2, high))), cols, write_z)

        def read_z(slot, row):
            return zx[slot, row * cols : (row + 1) * cols, :]

        for row in range(low + 1, high - 1):
            image = stencil_rows(lambda entry, cell: line[entry, cell, row : row + 1, :], OFF_ROW, read_z, row)
            for cell in range(CELLS):
                wx[k + 1, cell, row * cols : (row + 1) * cols, :] = image[cell]

    lane = lax.broadcasted_iota(jnp.int32, (8, LANES), 1)
    packed = jnp.zeros((8, LANES), jnp.float32)
    for tile in range(cols // 8):
        sums = [None] * 16
        for row in range(rows, 2 * rows):
            for cell in range(CELLS):
                at = row * cols + tile * 8
                w = [wx[k, cell, at : at + 8, :] for k in range(ITERS + 1)]
                for index, (i, j) in enumerate(PAIRS):
                    term = w[i] * w[j]
                    sums[index] = term if sums[index] is None else sums[index] + term
        sums[15] = jnp.zeros((8, LANES), jnp.float32)
        half = LANES // 2
        while len(sums) > 1:
            mask = (lane % (2 * half)) < half
            count = len(sums) // 2
            sums = [
                jnp.where(
                    mask,
                    sums[i] + roll(sums[i], -half),
                    sums[i + count] + roll(sums[i + count], half),
                )
                for i in range(count)
            ]
            half //= 2
        total = sums[0]
        while half >= 1:
            total = total + roll(total, -half)
            half //= 2
        packed = jnp.where(lane % 8 == tile, roll(total, tile), packed)
    lower = roll(roll(packed, 4, 0), 4)
    packed = jnp.where(lane % 8 < 4, packed, lower)[0:4, :]
    gram_out[...] = jnp.broadcast_to(packed[None], (peers, 4, LANES))


def weights_of(gram):
    g = {}
    for index, (i, j) in enumerate(PAIRS):
        value = roll(gram, -8 * index)
        g[i, j] = value
        g[j, i] = value
    upper = [
        [(g[i, j] + g[i + 1, j + 1]) + (g[i, j + 1] + g[i + 1, j]) for j in range(ITERS)] for i in range(ITERS)
    ]
    diag = [upper[i][i] for i in range(ITERS)]
    right = [g[0, i] + g[0, i + 1] for i in range(ITERS)]
    inverse = [None] * ITERS
    for k in range(ITERS):
        good = upper[k][k] > PIVOT_TOL * diag[k]
        inverse[k] = jnp.where(good, 1.0 / jnp.where(good, upper[k][k], 1.0), 0.0)
        for i in range(k + 1, ITERS):
            scale = upper[k][i] * inverse[k]
            for j in range(i, ITERS):
                upper[i][j] = upper[i][j] - scale * upper[k][j]
            right[i] = right[i] - scale * right[k]
    y = [None] * ITERS
    for k in reversed(range(ITERS)):
        value = right[k]
        for j in range(k + 1, ITERS):
            value = value - upper[k][j] * y[j]
        y[k] = value * inverse[k]
    return y


def update_kernel(shift_ref, gram_ref, z_ref, mine_ref, coefs_ref, *refs, step, first, last, rows, cols):
    if not first:
        refs = refs[1:]
    low_out, next_out, ux, yx, own, stage = refs
    total = gram_ref[0]
    for peer in range(1, gram_ref.shape[0]):
        total = total + gram_ref[peer]
    gram = jnp.concatenate([total, roll(total, -4)], axis=0)
    y = weights_of(gram)
    for k in range(ITERS):
        for tile in range(cols // 8):
            yx[k, tile * 8 : tile * 8 + 8, :] = jnp.broadcast_to(y[k][:, tile : tile + 1], (8, LANES))
    shift = shift_ref[step]
    for row in range(rows + 2):
        at = slice(row * cols, (row + 1) * cols)
        u = []
        for cell in range(CELLS):
            value = yx[0] * z_ref[0, cell, at, :]
            for k in range(1, ITERS):
                value = value + yx[k] * z_ref[k, cell, at, :]
            u.append(value)
        for slot, value in enumerate((roll(u[CELLS - 1], 1), *u, roll(u[0], -1))):
            ux[slot, at, :] = value

    def read_u(slot, row):
        return ux[slot, row * cols : (row + 1) * cols, :]

    double = 2.0 * shift
    for row in range(rows):
        image = stencil_rows(
            lambda entry, cell: coefs_ref[1, entry, cell, rows + row : rows + row + 1, :],
            range(len(OFFSETS)), read_u, row + 1,
        )
        for cell in range(CELLS):
            at = slice(row * cols, (row + 1) * cols)
            value = mine_ref[cell, at, :] - double * image[cell]
            if last:
                own[cell, at, :] = value
            else:
                next_out[cell, at, :] = value

    width = CELLS * LANES
    root = jnp.sqrt(jnp.broadcast_to(double, (1, LANES)))
    block = rows * cols
    tiles = from_chunks([root * ux[1 + cell, cols : cols + block, :] for cell in range(CELLS)], stage)
    for tile in range(len(tiles)):
        low_out[0, :, :, tile * LANES : (tile + 1) * LANES] = tiles[tile].reshape(rows, cols, LANES)
    if last:
        tiles = from_chunks([own[cell] for cell in range(CELLS)], stage)
        for tile in range(len(tiles)):
            next_out[:, :, tile * LANES : (tile + 1) * LANES] = tiles[tile].reshape(rows, cols, LANES)


def vmem():
    return pl.BlockSpec(memory_space=pltpu.VMEM)


def smem():
    return pl.BlockSpec(memory_space=pltpu.SMEM)


def shards(stiffness, mass, shifts, factor):
    rows, cols, width = factor.shape
    steps = shifts.shape[0]
    entries = len(OFFSETS)
    peers = lax.axis_size("rows")
    parity = (lax.axis_index("rows") % 2).astype(jnp.int32).reshape(1)
    block = rows * cols
    ext = 3 * rows
    ext_pad = -(-ext // 8) * 8
    f32 = jnp.float32

    within = [(i, i ^ 1) for i in range(peers) if i ^ 1 < peers]
    across = [(i, i + 1) for i in range(1, peers - 1, 2)]
    across = across + [(b, a) for a, b in across]

    def exchange(x):
        return lax.ppermute(x, "rows", within), lax.ppermute(x, "rows", across)

    mine = pl.pallas_call(
        pack_kernel,
        in_specs=[vmem(), vmem(), vmem()],
        out_specs=vmem(),
        out_shape=jax.ShapeDtypeStruct((CELLS, block + 2 * entries * rows, LANES), f32),
        scratch_shapes=[pltpu.VMEM((width, LANES), f32), pltpu.VMEM((LANES, width), f32)],
        compiler_params=params(),
        name="pack",
    )(stiffness, mass, factor)

    coefs = None
    lowrank = None
    for step in range(steps):
        even, odd = exchange(mine)
        coef_shape = jax.ShapeDtypeStruct((2, entries, CELLS, ext_pad, LANES), f32)
        out_shape = [
            jax.ShapeDtypeStruct((ITERS, CELLS, (rows + 2) * cols, LANES), f32),
            jax.ShapeDtypeStruct((peers, 4, LANES), f32),
        ]
        if step == 0:
            out_shape = [coef_shape] + out_shape
        outs = pl.pallas_call(
            functools.partial(
                krylov_kernel, step=step, first=step == 0, rows=rows, cols=cols, peers=peers
            ),
            in_specs=[smem(), smem(), vmem(), vmem(), vmem(), vmem()],
            out_specs=[vmem() for shape in out_shape],
            out_shape=out_shape,
            scratch_shapes=[
                pltpu.VMEM((ITERS + 1, CELLS, ext * cols, LANES), f32),
                pltpu.VMEM((CELLS + 2, ext * cols, LANES), f32),
                pltpu.VMEM((entries, CELLS, ext_pad, LANES), f32),
                pltpu.VMEM((LEVELS + 2 * level_count(), ext_pad, LANES), f32),
            ],
            compiler_params=params(),
            name=f"krylov{step}",
        )(parity, shifts, mine, even, odd, shifts.reshape(1, -1) if step == 0 else coefs)
        if step == 0:
            coefs = outs[0]
            outs = outs[1:]
        z, gram = outs
        gram = lax.all_to_all(gram, "rows", 0, 0)
        last = step + 1 == steps
        next_shape = (rows, cols, width) if last else (CELLS, block, LANES)
        out = pl.pallas_call(
            functools.partial(
                update_kernel, step=step, first=step == 0, last=last, rows=rows, cols=cols
            ),
            grid=(1,),
            in_specs=[smem(), vmem(), vmem(), vmem(), vmem()]
            + ([] if step == 0 else [pl.BlockSpec(memory_space=pl.ANY)]),
            out_specs=[
                pl.BlockSpec((1, rows, cols, width), lambda i, step=step: (step, 0, 0, 0)),
                vmem(),
            ],
            out_shape=[
                jax.ShapeDtypeStruct((steps, rows, cols, width), f32),
                jax.ShapeDtypeStruct(next_shape, f32),
            ],
            scratch_shapes=[
                pltpu.VMEM((CELLS + 2, (rows + 2) * cols, LANES), f32),
                pltpu.VMEM((ITERS, cols, LANES), f32),
                pltpu.VMEM((CELLS, block, LANES), f32),
                pltpu.VMEM((width, LANES), f32),
            ],
            input_output_aliases={} if step == 0 else {5: 0},
            compiler_params=params(),
            name=f"update{step}",
        )(*((shifts, gram, z, mine, coefs) + (() if step == 0 else (lowrank,))))
        lowrank, mine = out
    return lowrank, mine


def solution(mesh):
    in_specs = (P(None, "rows", None), P(None, "rows", None), P(), P("rows", None, None))
    out_specs = (P(None, "rows", None, None), P("rows", None, None))
    return jax.shard_map(shards, mesh=mesh, in_specs=in_specs, out_specs=out_specs, check_vma=False)
```

```python
import functools

import jax
import jax.numpy as jnp
from jax import lax
from jax.experimental import pallas as pl
from jax.experimental.pallas import tpu as pltpu
from jax.sharding import PartitionSpec as P

ITERS = 4
CELLS = 4
LANES = 128
PIVOT_TOL = 3e-7
OFFSETS = ((-1, -1), (-1, 0), (-1, 1), (0, -1), (0, 0), (0, 1), (1, -1), (1, 0), (1, 1))
OFF_ROW = (0, 1, 2, 6, 7, 8)
PAIRS = [(i, j) for i in range(ITERS + 1) for j in range(i, ITERS + 1)]

SUB = 8
DEPTH = LANES // SUB

E1, E2, G0, G1, G2, C0, C1, A3, L0, L1, L2, R0, R1, R2 = range(14)
PLANES = 14
TE, TINV, TH, TL, TR, TC3, TL0N, TR0N = range(8)
SINGLE = 8 * DEPTH
SA, SC, SB1, SF1, SB2, SF2, S4, SINV = range(8)
CHUNK_PLANES = SINGLE + 8


def roll(x, shift, axis=0):
    return pltpu.roll(x, shift % x.shape[axis], axis)


def params():
    return pltpu.CompilerParams(vmem_limit_bytes=40 * 1024 * 1024)


def to_chunks(natural, stage):
    for tile in range(CELLS):
        stage[tile * LANES : (tile + 1) * LANES, :] = natural[:, tile * LANES : (tile + 1) * LANES].T
    return [
        jnp.concatenate(
            [stage[pl.ds(depth * CELLS + cell, SUB, stride=CELLS * DEPTH), :] for depth in range(DEPTH)], axis=0
        ).T
        for cell in range(CELLS)
    ]


def from_chunks(planes, stage):
    for cell in range(CELLS):
        turned = planes[cell].T
        for depth in range(DEPTH):
            stage[pl.ds(depth * CELLS + cell, SUB, stride=CELLS * DEPTH), :] = turned[
                depth * SUB : (depth + 1) * SUB, :
            ]
    return [stage[tile * LANES : (tile + 1) * LANES, :].T for tile in range(CELLS)]


def split(matrix):
    return [matrix[depth * SUB : (depth + 1) * SUB, :] for depth in range(DEPTH)]


def next_chunk(registers):
    return registers[1:] + [roll(registers[0], -1)]


def previous_chunk(registers):
    return [roll(registers[-1], 1)] + registers[:-1]


def pack_kernel(shift_ref, stiff_ref, mass_ref, factor_ref, out_ref, shifts_out, stage, gather):
    rows, cols, width = factor_ref.shape
    for step in range(shifts_out.shape[0]):
        shifts_out[step] = jnp.full(shifts_out.shape[1:], shift_ref[step], jnp.float32)
    planes = to_chunks(factor_ref[...].reshape(rows * cols, width), stage)
    for cell in range(CELLS):
        out_ref[cell, 0 : rows * cols, :] = planes[cell]
    entries = len(OFFSETS)
    gather[...] = jnp.zeros(gather.shape, jnp.float32)
    for which, ref in enumerate((stiff_ref, mass_ref)):
        for entry in range(entries):
            at = (which * entries + entry) * rows
            gather[at : at + rows, :] = ref[entry]
    planes = to_chunks(gather[...], stage)
    count = 2 * entries * rows
    lane = lax.broadcasted_iota(jnp.int32, (count, LANES), 1)
    line = lax.broadcasted_iota(jnp.int32, (count, LANES), 0)
    column = (line // rows) % 3
    for cell in range(CELLS):
        plane = planes[cell][0:count, :]
        if cell == 0:
            plane = jnp.where((lane == 0) & (column == 0), 0.0, plane)
        if cell == CELLS - 1:
            plane = jnp.where((lane == LANES - 1) & (column == 2), 0.0, plane)
        out_ref[cell, rows * cols : rows * cols + count, :] = plane


def factor_chunks(group, below, center, above, c3, l0, r0, chunk):
    l0n, r0n = next_chunk(l0), next_chunk(r0)
    center = [center[v] + c3[v] * l0n[v] for v in range(DEPTH)]
    above = [c3[v] * r0n[v] for v in range(DEPTH)]

    def put(index, value):
        chunk[group, index] = value

    for v in range(DEPTH):
        put(TC3 * DEPTH + v, c3[v])
        put(TL0N * DEPTH + v, l0n[v])
        put(TR0N * DEPTH + v, r0n[v])
    last = DEPTH - 1
    inv, hi, left = [], [], []
    for v in range(last):
        if v == 0:
            inv.append(1.0 / center[0])
            left.append(-below[0])
        else:
            e = below[v] * inv[v - 1]
            put(TE * DEPTH + v, e)
            inv.append(1.0 / (center[v] - e * above[v - 1]))
            left.append(-e * left[v - 1])
        hi.append(above[v] * inv[v])
        put(TINV * DEPTH + v, inv[v])
        put(TH * DEPTH + v, hi[v])
    l = [None] * last
    r = [None] * last
    for v in reversed(range(last)):
        l[v] = left[v] * inv[v]
        if v == last - 1:
            r[v] = -hi[v]
        else:
            l[v] = l[v] - hi[v] * l[v + 1]
            r[v] = -hi[v] * r[v + 1]
        put(TL * DEPTH + v, l[v])
        put(TR * DEPTH + v, r[v])
    put(SINGLE + SA, below[last])
    put(SINGLE + SC, above[last])
    b = below[last] * l[last - 1]
    d = center[last] + below[last] * r[last - 1] + above[last] * roll(l[0], -1)
    f = above[last] * roll(r[0], -1)
    slot = SB1
    stride = 1
    while stride < SUB:
        inverse = 1.0 / d
        from_below = -b * roll(inverse, stride)
        from_above = -f * roll(inverse, -stride)
        d = d + from_below * roll(f, stride) + from_above * roll(b, -stride)
        b, f = from_below * roll(b, stride), from_above * roll(f, -stride)
        if 2 * stride == SUB:
            put(SINGLE + S4, from_below + from_above)
        else:
            put(SINGLE + slot, from_below)
            put(SINGLE + slot + 1, from_above)
            slot += 2
        stride *= 2
    put(SINGLE + SINV, 1.0 / d)


def solve_chunks(group, q, p0, chunk):
    def get(index):
        return chunk[group, index]

    p0n = next_chunk(p0)
    q = [q[v] - get(TC3 * DEPTH + v) * p0n[v] for v in range(DEPTH)]
    last = DEPTH - 1
    f = [q[0]]
    for v in range(1, last):
        f.append(q[v] - get(TE * DEPTH + v) * f[v - 1])
    p = [None] * last
    for v in reversed(range(last)):
        p[v] = f[v] * get(TINV * DEPTH + v)
        if v < last - 1:
            p[v] = p[v] - get(TH * DEPTH + v) * p[v + 1]
    s = q[last] - get(SINGLE + SA) * p[last - 1] - get(SINGLE + SC) * roll(p[0], -1)
    s = s + get(SINGLE + SB1) * roll(s, 1) + get(SINGLE + SF1) * roll(s, -1)
    s = s + get(SINGLE + SB2) * roll(s, 2) + get(SINGLE + SF2) * roll(s, -2)
    s = s + get(SINGLE + S4) * roll(s, 4)
    s = s * get(SINGLE + SINV)
    before = roll(s, 1)
    x = [p[v] + get(TL * DEPTH + v) * before + get(TR * DEPTH + v) * s for v in range(last)] + [s]
    xn = next_chunk(x)
    x0n = [p0n[v] + get(TL0N * DEPTH + v) * x[v] + get(TR0N * DEPTH + v) * xn[v] for v in range(DEPTH)]
    return x, previous_chunk(x), x0n


def build_factors(line, inner, chunk, rows, cols, ext):
    a = [line[3, cell, 0:ext, :] for cell in range(CELLS)]
    d = [line[4, cell, 0:ext, :] for cell in range(CELLS)]
    c = [line[5, cell, 0:ext, :] for cell in range(CELLS)]
    d = [jnp.where(x <= 0.0, 1.0, x) for x in d]
    g0 = 1.0 / d[0]
    e1 = a[1] * g0
    g1 = 1.0 / (d[1] - e1 * c[0])
    e2 = a[2] * g1
    g2 = 1.0 / (d[2] - e2 * c[1])
    f0 = -a[0]
    f1 = -e1 * f0
    f2 = -e2 * f1
    l2 = f2 * g2
    l1 = (f1 - c[1] * l2) * g1
    l0 = (f0 - c[0] * l1) * g0
    r2 = -c[2] * g2
    r1 = -c[1] * r2 * g1
    r0 = -c[0] * r1 * g0
    for index, value in (
        (E1, e1), (E2, e2), (G0, g0), (G1, g1), (G2, g2), (C0, c[0]), (C1, c[1]), (A3, a[3]),
        (L0, l0), (L1, l1), (L2, l2), (R0, r0), (R1, r1), (R2, r2),
    ):
        inner[index, 0:ext, :] = value
    planes = (a[3] * l2, d[3] + a[3] * r2, c[3], l0, r0)
    for group in range(ext // rows):
        turned = [
            split(
                jnp.concatenate(
                    [
                        jnp.broadcast_to(plane[row : row + 1, :], (cols, LANES))
                        for row in range(group * rows, (group + 1) * rows)
                    ],
                    axis=0,
                ).T
            )
            for plane in planes
        ]
        below, center, c3, l0t, r0t = turned
        factor_chunks(group, below, center, None, c3, l0t, r0t, chunk)


def stencil_rows(coef, entries, read, row):
    out = []
    for cell in range(CELLS):
        total = None
        for entry in entries:
            offset = OFFSETS[entry]
            term = coef(entry, cell) * read(1 + cell + offset[1], row + offset[0])
            total = term if total is None else total + term
        out.append(total)
    return out


def krylov_kernel(
    parity_ref, shift_ref, mine_ref, even_ref, odd_ref, *refs, step, first, rows, cols, peers
):
    if first:
        coefs_ref, z_out, gram_out, wx, zx, line, inner, chunk, px, qx, sums = refs
    else:
        coefs_ref, z_out, gram_out, wx, zx, line, inner, chunk, px, qx, sums = refs
    ext = 3 * rows
    entries = len(OFFSETS)
    block = rows * cols
    parity = parity_ref[0]
    at_even = jnp.where(parity == 0, 2 * rows, 0)
    at_odd = 2 * rows - at_even
    wx[0, :, pl.ds(rows * cols, block), :] = mine_ref[:, 0:block, :]
    wx[0, :, pl.ds(pl.multiple_of(at_even * cols, cols), block), :] = even_ref[:, 0:block, :]
    wx[0, :, pl.ds(pl.multiple_of(at_odd * cols, cols), block), :] = odd_ref[:, 0:block, :]
    if first:
        low_is_even = parity == 1
        for which in range(2):
            for entry in range(entries):
                at = block + (which * entries + entry) * rows
                for cell in range(CELLS):
                    even = even_ref[cell, at : at + rows, :]
                    odd = odd_ref[cell, at : at + rows, :]
                    coefs_ref[which, entry, cell, 0:rows, :] = jnp.where(low_is_even, even, odd)
                    coefs_ref[which, entry, cell, rows : 2 * rows, :] = mine_ref[cell, at : at + rows, :]
                    coefs_ref[which, entry, cell, 2 * rows : ext, :] = jnp.where(low_is_even, odd, even)
    shift = shift_ref[step, 0:1, :]
    for entry in range(entries):
        for cell in range(CELLS):
            line[entry, cell, 0:ext, :] = (
                coefs_ref[0, entry, cell, 0:ext, :] + shift * coefs_ref[1, entry, cell, 0:ext, :]
            )
    build_factors(line, inner, chunk, rows, cols, ext)

    def span(row, count=1):
        return slice(row * cols, (row + count) * cols)

    for k in range(ITERS):
        low, high = k, ext - k

        def coef(index, row):
            return inner[index, row : row + 1, :]

        for group in range(ext // rows):
            wanted = [row for row in range(group * rows, (group + 1) * rows) if low <= row < high]
            for row in wanted:
                v0, v1, v2, v3 = (wx[k, cell, span(row), :] for cell in range(CELLS))
                f1 = v1 - coef(E1, row) * v0
                f2 = v2 - coef(E2, row) * f1
                x2 = f2 * coef(G2, row)
                x1 = (f1 - coef(C1, row) * x2) * coef(G1, row)
                x0 = (v0 - coef(C0, row) * x1) * coef(G0, row)
                px[0, span(row), :] = x0
                px[1, span(row), :] = x1
                px[2, span(row), :] = x2
                qx[span(row), :] = v3 - coef(A3, row) * x2
            at = span(group * rows, rows)
            x, before, after = solve_chunks(group, split(qx[at, :].T), split(px[0, at, :].T), chunk)
            zx[CELLS, at, :] = jnp.concatenate(x, axis=0).T
            zx[0, at, :] = jnp.concatenate(before, axis=0).T
            zx[CELLS + 1, at, :] = jnp.concatenate(after, axis=0).T
            for row in wanted:
                x3 = zx[CELLS, span(row), :]
                x3b = zx[0, span(row), :]
                for cell in range(CELLS - 1):
                    zx[1 + cell, span(row), :] = (
                        px[cell, span(row), :] + coef(L0 + cell, row) * x3b + coef(R0 + cell, row) * x3
                    )
                if rows - 1 <= row <= 2 * rows:
                    for slot in range(CELLS + 2):
                        z_out[k, slot, span(row - rows + 1), :] = zx[slot, span(row), :]

        def read_z(slot, row):
            return zx[slot, span(row), :]

        for row in range(low + 1, high - 1):
            image = stencil_rows(lambda entry, cell: line[entry, cell, row : row + 1, :], OFF_ROW, read_z, row)
            for cell in range(CELLS):
                wx[k + 1, cell, span(row), :] = image[cell]

    for tile in range(cols // 8):
        total = [None] * len(PAIRS)
        for row in range(rows, 2 * rows):
            for cell in range(CELLS):
                at = row * cols + tile * 8
                w = [wx[k, cell, at : at + 8, :] for k in range(ITERS + 1)]
                for index, (i, j) in enumerate(PAIRS):
                    term = w[i] * w[j]
                    total[index] = term if total[index] is None else total[index] + term
        for index in range(len(PAIRS)):
            sums[index * cols + tile * 8 : index * cols + tile * 8 + 8, :] = total[index]
    sums[len(PAIRS) * cols :, :] = jnp.zeros((sums.shape[0] - len(PAIRS) * cols, LANES), jnp.float32)
    for part in range(sums.shape[0] // LANES):
        turned = sums[part * LANES : (part + 1) * LANES, :].T
        gram_out[:, part : part + 1, :] = jnp.broadcast_to(
            jnp.sum(turned, axis=0, keepdims=True)[None], (peers, 1, LANES)
        )


def weights_of(g):
    upper = [
        [(g[i, j] + g[i + 1, j + 1]) + (g[i, j + 1] + g[i + 1, j]) for j in range(ITERS)] for i in range(ITERS)
    ]
    diag = [upper[i][i] for i in range(ITERS)]
    right = [g[0, i] + g[0, i + 1] for i in range(ITERS)]
    inverse = [None] * ITERS
    for k in range(ITERS):
        good = upper[k][k] > PIVOT_TOL * diag[k]
        inverse[k] = jnp.where(good, 1.0 / jnp.where(good, upper[k][k], 1.0), 0.0)
        for i in range(k + 1, ITERS):
            scale = upper[k][i] * inverse[k]
            for j in range(i, ITERS):
                upper[i][j] = upper[i][j] - scale * upper[k][j]
            right[i] = right[i] - scale * right[k]
    y = [None] * ITERS
    for k in reversed(range(ITERS)):
        value = right[k]
        for j in range(k + 1, ITERS):
            value = value - upper[k][j] * y[j]
        y[k] = value * inverse[k]
    return y


def update_kernel(shift_ref, gram_ref, z_ref, mine_ref, coefs_ref, *refs, step, first, last, rows, cols):
    if not first:
        refs = refs[1:]
    low_out, next_out, ux, yx, own, stage = refs
    total = gram_ref[0]
    for peer in range(1, gram_ref.shape[0]):
        total = total + gram_ref[peer]
    g = {}
    per_part = LANES // cols
    for part in range(total.shape[0]):
        turned = jnp.broadcast_to(total[part : part + 1, :], (LANES, LANES)).T
        for index, (i, j) in enumerate(PAIRS[part * per_part : (part + 1) * per_part]):
            g[i, j] = g[j, i] = turned[index * cols : (index + 1) * cols, :]
    y = weights_of(g)
    for k in range(ITERS):
        yx[k] = y[k]

    def span(row, count=1):
        return slice(row * cols, (row + count) * cols)

    for row in range(rows + 2):
        for slot in range(CELLS + 2):
            value = yx[0] * z_ref[0, slot, span(row), :]
            for k in range(1, ITERS):
                value = value + yx[k] * z_ref[k, slot, span(row), :]
            ux[slot, span(row), :] = value

    def read_u(slot, row):
        return ux[slot, span(row), :]

    double = 2.0 * shift_ref[step, 0:1, :]
    for row in range(rows):
        image = stencil_rows(
            lambda entry, cell: coefs_ref[1, entry, cell, rows + row : rows + row + 1, :],
            range(len(OFFSETS)), read_u, row + 1,
        )
        for cell in range(CELLS):
            value = mine_ref[cell, span(row), :] - double * image[cell]
            if last:
                own[cell, span(row), :] = value
            else:
                next_out[cell, span(row), :] = value

    root = jnp.sqrt(double)
    tiles = from_chunks([root * ux[1 + cell, span(1, rows), :] for cell in range(CELLS)], stage)
    for tile in range(len(tiles)):
        low_out[0, :, :, tile * LANES : (tile + 1) * LANES] = tiles[tile].reshape(rows, cols, LANES)
    if last:
        tiles = from_chunks([own[cell] for cell in range(CELLS)], stage)
        for tile in range(len(tiles)):
            next_out[:, :, tile * LANES : (tile + 1) * LANES] = tiles[tile].reshape(rows, cols, LANES)


def vmem():
    return pl.BlockSpec(memory_space=pltpu.VMEM)


def smem():
    return pl.BlockSpec(memory_space=pltpu.SMEM)


def shards(stiffness, mass, shifts, factor):
    rows, cols, width = factor.shape
    steps = shifts.shape[0]
    entries = len(OFFSETS)
    peers = lax.axis_size("rows")
    parity = (lax.axis_index("rows") % 2).astype(jnp.int32).reshape(1)
    block = rows * cols
    ext = 3 * rows
    ext_pad = -(-ext // 8) * 8
    f32 = jnp.float32
    gram_rows = -(-len(PAIRS) * cols // LANES)
    assert block == LANES and width == CELLS * LANES

    within = [(i, i ^ 1) for i in range(peers) if i ^ 1 < peers]
    across = [(i, i + 1) for i in range(1, peers - 1, 2)]
    across = across + [(b, a) for a, b in across]

    def exchange(x):
        return lax.ppermute(x, "rows", within), lax.ppermute(x, "rows", across)

    whole = pl.BlockSpec
    mine, shift_rows = pl.pallas_call(
        pack_kernel,
        grid=(1,),
        in_specs=[
            smem(),
            whole(stiffness.shape, lambda i: (0, 0, 0)),
            whole(mass.shape, lambda i: (0, 0, 0)),
            whole(factor.shape, lambda i: (0, 0, 0)),
        ],
        out_specs=[vmem(), vmem()],
        out_shape=[
            jax.ShapeDtypeStruct((CELLS, block + 2 * entries * rows, LANES), f32),
            jax.ShapeDtypeStruct((steps, 8, LANES), f32),
        ],
        scratch_shapes=[pltpu.VMEM((width, LANES), f32), pltpu.VMEM((LANES, width), f32)],
        compiler_params=params(),
        name="pack",
    )(shifts, stiffness, mass, factor)

    coefs = None
    lowrank = None
    for step in range(steps):
        first = step == 0
        even, odd = exchange(mine)
        coef_shape = jax.ShapeDtypeStruct((2, entries, CELLS, ext_pad, LANES), f32)
        out_shape = [
            jax.ShapeDtypeStruct((ITERS, CELLS + 2, (rows + 2) * cols, LANES), f32),
            jax.ShapeDtypeStruct((peers, gram_rows, LANES), f32),
        ]
        if first:
            out_shape = [coef_shape] + out_shape
        outs = pl.pallas_call(
            functools.partial(krylov_kernel, step=step, first=first, rows=rows, cols=cols, peers=peers),
            in_specs=[smem()] + [vmem()] * (4 if first else 5),
            out_specs=[vmem() for shape in out_shape],
            out_shape=out_shape,
            scratch_shapes=[
                pltpu.VMEM((ITERS + 1, CELLS, ext * cols, LANES), f32),
                pltpu.VMEM((CELLS + 2, ext * cols, LANES), f32),
                pltpu.VMEM((entries, CELLS, ext_pad, LANES), f32),
                pltpu.VMEM((PLANES, ext_pad, LANES), f32),
                pltpu.VMEM((3, CHUNK_PLANES, SUB, LANES), f32),
                pltpu.VMEM((CELLS - 1, ext * cols, LANES), f32),
                pltpu.VMEM((ext * cols, LANES), f32),
                pltpu.VMEM((gram_rows * LANES, LANES), f32),
            ],
            compiler_params=params(),
            name=f"krylov{step}",
        )(*((parity, shift_rows, mine, even, odd) + (() if first else (coefs,))))
        if first:
            coefs = outs[0]
            outs = outs[1:]
        z, gram = outs
        gram = lax.all_to_all(gram, "rows", 0, 0)
        last = step + 1 == steps
        next_shape = (rows, cols, width) if last else (CELLS, block, LANES)
        lowrank, mine = pl.pallas_call(
            functools.partial(update_kernel, step=step, first=first, last=last, rows=rows, cols=cols),
            grid=(1,),
            in_specs=[vmem()] * 5 + ([] if first else [pl.BlockSpec(memory_space=pl.ANY)]),
            out_specs=[
                pl.BlockSpec((1, rows, cols, width), lambda i, step=step: (step, 0, 0, 0)),
                vmem(),
            ],
            out_shape=[
                jax.ShapeDtypeStruct((steps, rows, cols, width), f32),
                jax.ShapeDtypeStruct(next_shape, f32),
            ],
            scratch_shapes=[
                pltpu.VMEM((CELLS + 2, (rows + 2) * cols, LANES), f32),
                pltpu.VMEM((ITERS, cols, LANES), f32),
                pltpu.VMEM((CELLS, block, LANES), f32),
                pltpu.VMEM((width, LANES), f32),
            ],
            input_output_aliases={} if first else {5: 0},
            compiler_params=params(),
            name=f"update{step}",
        )(*((shift_rows, gram, z, mine, coefs) + (() if first else (lowrank,))))
    return lowrank, mine


def solution(mesh):
    in_specs = (P(None, "rows", None), P(None, "rows", None), P(), P("rows", None, None))
    out_specs = (P(None, "rows", None, None), P("rows", None, None))
    return jax.shard_map(shards, mesh=mesh, in_specs=in_specs, out_specs=out_specs, check_vma=False)
```

```python
import functools

import jax
import jax.numpy as jnp
from jax import lax
from jax.experimental import pallas as pl
from jax.experimental.pallas import tpu as pltpu
from jax.sharding import PartitionSpec as P

ITERS = 4
CELLS = 4
LANES = 128
PIVOT_TOL = 3e-7
OFFSETS = ((-1, -1), (-1, 0), (-1, 1), (0, -1), (0, 0), (0, 1), (1, -1), (1, 0), (1, 1))
OFF_ROW = (0, 1, 2, 6, 7, 8)
PAIRS = [(i, j) for i in range(ITERS + 1) for j in range(i, ITERS + 1)]

SUB = 8
DEPTH = LANES // SUB

E1, E2, G0, G1, G2, C0, C1, A3, L0, L1, L2, R0, R1, R2 = range(14)
PLANES = 14
TE, TINV, TH, TL, TR, TC3, TL0N, TR0N = range(8)
SINGLE = 8 * DEPTH
SA, SC, SB1, SF1, SB2, SF2, S4, SINV = range(8)
CHUNK_PLANES = SINGLE + 8


def roll(x, shift, axis=0):
    return pltpu.roll(x, shift % x.shape[axis], axis)


def params():
    return pltpu.CompilerParams(vmem_limit_bytes=40 * 1024 * 1024)


def to_chunks(natural, stage):
    for tile in range(CELLS):
        stage[tile * LANES : (tile + 1) * LANES, :] = natural[:, tile * LANES : (tile + 1) * LANES].T
    return [
        jnp.concatenate(
            [stage[pl.ds(depth * CELLS + cell, SUB, stride=CELLS * DEPTH), :] for depth in range(DEPTH)], axis=0
        ).T
        for cell in range(CELLS)
    ]


def from_chunks(planes, stage):
    for cell in range(CELLS):
        turned = planes[cell].T
        for depth in range(DEPTH):
            stage[pl.ds(depth * CELLS + cell, SUB, stride=CELLS * DEPTH), :] = turned[
                depth * SUB : (depth + 1) * SUB, :
            ]
    return [stage[tile * LANES : (tile + 1) * LANES, :].T for tile in range(CELLS)]


def split(matrix):
    return [matrix[depth * SUB : (depth + 1) * SUB, :] for depth in range(DEPTH)]


def next_chunk(registers):
    return registers[1:] + [roll(registers[0], -1)]


def previous_chunk(registers):
    return [roll(registers[-1], 1)] + registers[:-1]


def pack_kernel(
    shift_hbm, stiff_hbm, mass_hbm, factor_hbm, out_ref, shifts_out,
    stage, gather, shift_ref, stiff_ref, mass_ref, factor_ref, shift_sem, stiff_sem, mass_sem, factor_sem,
):
    copies = [
        pltpu.make_async_copy(*operands)
        for operands in (
            (factor_hbm, factor_ref, factor_sem),
            (stiff_hbm, stiff_ref, stiff_sem),
            (mass_hbm, mass_ref, mass_sem),
            (shift_hbm, shift_ref, shift_sem),
        )
    ]
    for copy in copies:
        copy.start()
    rows, cols, width = factor_ref.shape
    entries = len(OFFSETS)
    gather[...] = jnp.zeros(gather.shape, jnp.float32)
    copies[0].wait()
    planes = to_chunks(factor_ref[...].reshape(rows * cols, width), stage)
    for cell in range(CELLS):
        out_ref[cell, 0 : rows * cols, :] = planes[cell]
    for which, ref in enumerate((stiff_ref, mass_ref)):
        copies[1 + which].wait()
        for entry in range(entries):
            at = (which * entries + entry) * rows
            gather[at : at + rows, :] = ref[entry]
    planes = to_chunks(gather[...], stage)
    count = 2 * entries * rows
    lane = lax.broadcasted_iota(jnp.int32, (count, LANES), 1)
    line = lax.broadcasted_iota(jnp.int32, (count, LANES), 0)
    column = (line // rows) % 3
    for cell in range(CELLS):
        plane = planes[cell][0:count, :]
        if cell == 0:
            plane = jnp.where((lane == 0) & (column == 0), 0.0, plane)
        if cell == CELLS - 1:
            plane = jnp.where((lane == LANES - 1) & (column == 2), 0.0, plane)
        out_ref[cell, rows * cols : rows * cols + count, :] = plane
    copies[3].wait()
    for step in range(shifts_out.shape[0]):
        shifts_out[step] = jnp.full(shifts_out.shape[1:], shift_ref[step], jnp.float32)


def factor_chunks(group, below, center, above, c3, l0, r0, chunk):
    l0n, r0n = next_chunk(l0), next_chunk(r0)
    center = [center[v] + c3[v] * l0n[v] for v in range(DEPTH)]
    above = [c3[v] * r0n[v] for v in range(DEPTH)]

    def put(index, value):
        chunk[group, index] = value

    for v in range(DEPTH):
        put(TC3 * DEPTH + v, c3[v])
        put(TL0N * DEPTH + v, l0n[v])
        put(TR0N * DEPTH + v, r0n[v])
    last = DEPTH - 1
    inv, hi, left = [], [], []
    for v in range(last):
        if v == 0:
            inv.append(1.0 / center[0])
            left.append(-below[0])
        else:
            e = below[v] * inv[v - 1]
            put(TE * DEPTH + v, e)
            inv.append(1.0 / (center[v] - e * above[v - 1]))
            left.append(-e * left[v - 1])
        hi.append(above[v] * inv[v])
        put(TINV * DEPTH + v, inv[v])
        put(TH * DEPTH + v, hi[v])
    l = [None] * last
    r = [None] * last
    for v in reversed(range(last)):
        l[v] = left[v] * inv[v]
        if v == last - 1:
            r[v] = -hi[v]
        else:
            l[v] = l[v] - hi[v] * l[v + 1]
            r[v] = -hi[v] * r[v + 1]
        put(TL * DEPTH + v, l[v])
        put(TR * DEPTH + v, r[v])
    put(SINGLE + SA, below[last])
    put(SINGLE + SC, above[last])
    b = below[last] * l[last - 1]
    d = center[last] + below[last] * r[last - 1] + above[last] * roll(l[0], -1)
    f = above[last] * roll(r[0], -1)
    slot = SB1
    stride = 1
    while stride < SUB:
        inverse = 1.0 / d
        from_below = -b * roll(inverse, stride)
        from_above = -f * roll(inverse, -stride)
        d = d + from_below * roll(f, stride) + from_above * roll(b, -stride)
        b, f = from_below * roll(b, stride), from_above * roll(f, -stride)
        if 2 * stride == SUB:
            put(SINGLE + S4, from_below + from_above)
        else:
            put(SINGLE + slot, from_below)
            put(SINGLE + slot + 1, from_above)
            slot += 2
        stride *= 2
    put(SINGLE + SINV, 1.0 / d)


def solve_chunks(group, q, p0, chunk):
    def get(index):
        return chunk[group, index]

    p0n = next_chunk(p0)
    q = [q[v] - get(TC3 * DEPTH + v) * p0n[v] for v in range(DEPTH)]
    last = DEPTH - 1
    f = [q[0]]
    for v in range(1, last):
        f.append(q[v] - get(TE * DEPTH + v) * f[v - 1])
    p = [None] * last
    for v in reversed(range(last)):
        p[v] = f[v] * get(TINV * DEPTH + v)
        if v < last - 1:
            p[v] = p[v] - get(TH * DEPTH + v) * p[v + 1]
    s = q[last] - get(SINGLE + SA) * p[last - 1] - get(SINGLE + SC) * roll(p[0], -1)
    s = s + get(SINGLE + SB1) * roll(s, 1) + get(SINGLE + SF1) * roll(s, -1)
    s = s + get(SINGLE + SB2) * roll(s, 2) + get(SINGLE + SF2) * roll(s, -2)
    s = s + get(SINGLE + S4) * roll(s, 4)
    s = s * get(SINGLE + SINV)
    before = roll(s, 1)
    x = [p[v] + get(TL * DEPTH + v) * before + get(TR * DEPTH + v) * s for v in range(last)] + [s]
    xn = next_chunk(x)
    x0n = [p0n[v] + get(TL0N * DEPTH + v) * x[v] + get(TR0N * DEPTH + v) * xn[v] for v in range(DEPTH)]
    return x, previous_chunk(x), x0n


def build_lines(coefs_ref, shift, line, ext):
    for entry in range(len(OFFSETS)):
        for cell in range(CELLS):
            line[entry, cell, 0:ext, :] = (
                coefs_ref[0, entry, cell, 0:ext, :] + shift * coefs_ref[1, entry, cell, 0:ext, :]
            )


def build_factors(line, inner, chunk, rows, cols, ext):
    a = [line[3, cell, 0:ext, :] for cell in range(CELLS)]
    d = [line[4, cell, 0:ext, :] for cell in range(CELLS)]
    c = [line[5, cell, 0:ext, :] for cell in range(CELLS)]
    d = [jnp.where(x <= 0.0, 1.0, x) for x in d]
    g0 = 1.0 / d[0]
    e1 = a[1] * g0
    g1 = 1.0 / (d[1] - e1 * c[0])
    e2 = a[2] * g1
    g2 = 1.0 / (d[2] - e2 * c[1])
    f0 = -a[0]
    f1 = -e1 * f0
    f2 = -e2 * f1
    l2 = f2 * g2
    l1 = (f1 - c[1] * l2) * g1
    l0 = (f0 - c[0] * l1) * g0
    r2 = -c[2] * g2
    r1 = -c[1] * r2 * g1
    r0 = -c[0] * r1 * g0
    for index, value in (
        (E1, e1), (E2, e2), (G0, g0), (G1, g1), (G2, g2), (C0, c[0]), (C1, c[1]), (A3, a[3]),
        (L0, l0), (L1, l1), (L2, l2), (R0, r0), (R1, r1), (R2, r2),
    ):
        inner[index, 0:ext, :] = value
    planes = (a[3] * l2, d[3] + a[3] * r2, c[3], l0, r0)
    for group in range(ext // rows):
        turned = [
            split(
                jnp.concatenate(
                    [
                        jnp.broadcast_to(plane[row : row + 1, :], (cols, LANES))
                        for row in range(group * rows, (group + 1) * rows)
                    ],
                    axis=0,
                ).T
            )
            for plane in planes
        ]
        below, center, c3, l0t, r0t = turned
        factor_chunks(group, below, center, None, c3, l0t, r0t, chunk)


def stencil_rows(coef, entries, read, row):
    out = []
    for cell in range(CELLS):
        total = None
        for entry in entries:
            offset = OFFSETS[entry]
            term = coef(entry, cell) * read(1 + cell + offset[1], row + offset[0])
            total = term if total is None else total + term
        out.append(total)
    return out


def line_solve(group, wanted, read, inner, chunk, px, qx, zx, base, rows, cols):
    def coef(index, row):
        return inner[index, row : row + 1, :]

    def span(row, count=1):
        return slice((row - base) * cols, (row - base + count) * cols)

    for row in wanted:
        v0, v1, v2, v3 = (read(cell, row) for cell in range(CELLS))
        f1 = v1 - coef(E1, row) * v0
        f2 = v2 - coef(E2, row) * f1
        x2 = f2 * coef(G2, row)
        x1 = (f1 - coef(C1, row) * x2) * coef(G1, row)
        x0 = (v0 - coef(C0, row) * x1) * coef(G0, row)
        px[0, span(row), :] = x0
        px[1, span(row), :] = x1
        px[2, span(row), :] = x2
        qx[span(row), :] = v3 - coef(A3, row) * x2
    at = span(group * rows, rows)
    x, before, after = solve_chunks(group, split(qx[at, :].T), split(px[0, at, :].T), chunk)
    zx[CELLS, at, :] = jnp.concatenate(x, axis=0).T
    zx[0, at, :] = jnp.concatenate(before, axis=0).T
    zx[CELLS + 1, at, :] = jnp.concatenate(after, axis=0).T
    for row in wanted:
        x3 = zx[CELLS, span(row), :]
        x3b = zx[0, span(row), :]
        for cell in range(CELLS - 1):
            zx[1 + cell, span(row), :] = (
                px[cell, span(row), :] + coef(L0 + cell, row) * x3b + coef(R0 + cell, row) * x3
            )


def side_kernel(shift_ref, coefs_ref, mine_ref, u_ref, *refs, step, rows, cols):
    low_out, line, inner, chunk, z_out, px, qx, stage = refs[-8:]
    ext = 3 * rows
    build_lines(coefs_ref, shift_ref[step + 1, 0:1, :], line, ext)
    build_factors(line, inner, chunk, rows, cols, ext)

    def read(cell, row):
        return mine_ref[cell, (row - rows) * cols : (row - rows + 1) * cols, :]

    line_solve(1, list(range(rows, 2 * rows)), read, inner, chunk, px, qx, z_out, rows, rows, cols)
    root = jnp.sqrt(2.0 * shift_ref[step, 0:1, :])
    write_natural(low_out, 0, [root * u_ref[cell] for cell in range(CELLS)], stage, rows, cols)


def write_natural(out, lead, planes, stage, rows, cols):
    tiles = from_chunks(planes, stage)
    for tile in range(len(tiles)):
        value = tiles[tile].reshape(rows, cols, LANES)
        if lead is None:
            out[:, :, tile * LANES : (tile + 1) * LANES] = value
        else:
            out[lead, :, :, tile * LANES : (tile + 1) * LANES] = value


def krylov_kernel(
    parity_ref, shift_ref, mine_ref, even_ref, odd_ref, *refs, step, first, rows, cols, peers
):
    if first:
        coefs_ref, z_out, gram_out, wx, zx, px, qx, sums, line, inner, chunk = refs
    else:
        line, inner, chunk, z_mine, z_out, gram_out, wx, zx, px, qx, sums = refs
    ext = 3 * rows
    entries = len(OFFSETS)
    block = rows * cols
    parity = parity_ref[0]
    at_even = jnp.where(parity == 0, 2 * rows, 0)
    at_odd = 2 * rows - at_even
    wx[0, :, pl.ds(rows * cols, block), :] = mine_ref[:, 0:block, :]
    wx[0, :, pl.ds(pl.multiple_of(at_even * cols, cols), block), :] = even_ref[:, 0:block, :]
    wx[0, :, pl.ds(pl.multiple_of(at_odd * cols, cols), block), :] = odd_ref[:, 0:block, :]
    if first:
        low_is_even = parity == 1
        for which in range(2):
            for entry in range(entries):
                at = block + (which * entries + entry) * rows
                for cell in range(CELLS):
                    even = even_ref[cell, at : at + rows, :]
                    odd = odd_ref[cell, at : at + rows, :]
                    coefs_ref[which, entry, cell, 0:rows, :] = jnp.where(low_is_even, even, odd)
                    coefs_ref[which, entry, cell, rows : 2 * rows, :] = mine_ref[cell, at : at + rows, :]
                    coefs_ref[which, entry, cell, 2 * rows : ext, :] = jnp.where(low_is_even, odd, even)
        build_lines(coefs_ref, shift_ref[step, 0:1, :], line, ext)
        build_factors(line, inner, chunk, rows, cols, ext)

    def span(row, count=1):
        return slice(row * cols, (row + count) * cols)

    for k in range(ITERS):
        low, high = k, ext - k

        def read_w(cell, row):
            return wx[k, cell, span(row), :]

        for group in range(ext // rows):
            if k == 0 and group == 1 and not first:
                zx[:, span(rows, rows), :] = z_mine[...]
                continue
            wanted = [row for row in range(group * rows, (group + 1) * rows) if low <= row < high]
            line_solve(group, wanted, read_w, inner, chunk, px, qx, zx, 0, rows, cols)
        for row in range(rows - 1, 2 * rows + 1):
            z_out[k, :, span(row - rows + 1), :] = zx[:, span(row), :]

        def read_z(slot, row):
            return zx[slot, span(row), :]

        for row in range(low + 1, high - 1):
            image = stencil_rows(lambda entry, cell: line[entry, cell, row : row + 1, :], OFF_ROW, read_z, row)
            for cell in range(CELLS):
                wx[k + 1, cell, span(row), :] = image[cell]

    for tile in range(cols // 8):
        total = [None] * len(PAIRS)
        for row in range(rows, 2 * rows):
            for cell in range(CELLS):
                at = row * cols + tile * 8
                w = [wx[k, cell, at : at + 8, :] for k in range(ITERS + 1)]
                for index, (i, j) in enumerate(PAIRS):
                    term = w[i] * w[j]
                    total[index] = term if total[index] is None else total[index] + term
        for index in range(len(PAIRS)):
            sums[index * cols + tile * 8 : index * cols + tile * 8 + 8, :] = total[index]
    sums[len(PAIRS) * cols :, :] = jnp.zeros((sums.shape[0] - len(PAIRS) * cols, LANES), jnp.float32)
    for part in range(sums.shape[0] // LANES):
        turned = sums[part * LANES : (part + 1) * LANES, :].T
        gram_out[:, part : part + 1, :] = jnp.broadcast_to(
            jnp.sum(turned, axis=0, keepdims=True)[None], (peers, 1, LANES)
        )


def weights_of(g):
    upper = [
        [(g[i, j] + g[i + 1, j + 1]) + (g[i, j + 1] + g[i + 1, j]) for j in range(ITERS)] for i in range(ITERS)
    ]
    diag = [upper[i][i] for i in range(ITERS)]
    right = [g[0, i] + g[0, i + 1] for i in range(ITERS)]
    inverse = [None] * ITERS
    for k in range(ITERS):
        good = upper[k][k] > PIVOT_TOL * diag[k]
        inverse[k] = jnp.where(good, 1.0 / jnp.where(good, upper[k][k], 1.0), 0.0)
        for i in range(k + 1, ITERS):
            scale = upper[k][i] * inverse[k]
            for j in range(i, ITERS):
                upper[i][j] = upper[i][j] - scale * upper[k][j]
            right[i] = right[i] - scale * right[k]
    y = [None] * ITERS
    for k in reversed(range(ITERS)):
        value = right[k]
        for j in range(k + 1, ITERS):
            value = value - upper[k][j] * y[j]
        y[k] = value * inverse[k]
    return y


def update_kernel(shift_ref, gram_ref, z_ref, mine_ref, coefs_ref, *refs, step, last, rows, cols):
    low_out, next_out, ux, yx, own, stage = refs[-6:]
    parts = [gram_ref[peer] for peer in range(gram_ref.shape[0])]
    while len(parts) > 1:
        parts = [a + b for a, b in zip(parts[0::2], parts[1::2])] + parts[len(parts) // 2 * 2 :]
    total = parts[0]
    g = {}
    per_part = LANES // cols
    for part in range(total.shape[0]):
        turned = jnp.broadcast_to(total[part : part + 1, :], (LANES, LANES)).T
        for index, (i, j) in enumerate(PAIRS[part * per_part : (part + 1) * per_part]):
            g[i, j] = g[j, i] = turned[index * cols : (index + 1) * cols, :]
    y = weights_of(g)
    for k in range(ITERS):
        yx[k] = y[k]

    def span(row, count=1):
        return slice(row * cols, (row + count) * cols)

    for row in range(rows + 2):
        for slot in range(CELLS + 2):
            value = yx[0] * z_ref[0, slot, span(row), :]
            for k in range(1, ITERS):
                value = value + yx[k] * z_ref[k, slot, span(row), :]
            ux[slot, span(row), :] = value
            if not last and 0 < row <= rows and 0 < slot <= CELLS:
                low_out[slot - 1, span(row - 1), :] = value

    def read_u(slot, row):
        return ux[slot, span(row), :]

    double = 2.0 * shift_ref[step, 0:1, :]
    for row in range(rows):
        image = stencil_rows(
            lambda entry, cell: coefs_ref[1, entry, cell, rows + row : rows + row + 1, :],
            range(len(OFFSETS)), read_u, row + 1,
        )
        for cell in range(CELLS):
            value = mine_ref[cell, span(row), :] - double * image[cell]
            if last:
                own[cell, span(row), :] = value
            else:
                next_out[cell, span(row), :] = value
    if last:
        root = jnp.sqrt(double)
        planes = [root * ux[1 + cell, span(1, rows), :] for cell in range(CELLS)]
        write_natural(low_out, 0, planes, stage, rows, cols)
        write_natural(next_out, None, [own[cell] for cell in range(CELLS)], stage, rows, cols)


def vmem():
    return pl.BlockSpec(memory_space=pltpu.VMEM)


def low_block(steps, rows, cols, width, step):
    return pl.BlockSpec((1, rows, cols, width), lambda i: (step, 0, 0, 0))


def smem():
    return pl.BlockSpec(memory_space=pltpu.SMEM)


def shards(stiffness, mass, shifts, factor):
    rows, cols, width = factor.shape
    steps = shifts.shape[0]
    entries = len(OFFSETS)
    peers = lax.axis_size("rows")
    parity = (lax.axis_index("rows") % 2).astype(jnp.int32).reshape(1)
    block = rows * cols
    ext = 3 * rows
    ext_pad = -(-ext // 8) * 8
    f32 = jnp.float32
    gram_rows = -(-len(PAIRS) * cols // LANES)
    assert block == LANES and width == CELLS * LANES

    within = [(i, i ^ 1) for i in range(peers) if i ^ 1 < peers]
    across = [(i, i + 1) for i in range(1, peers - 1, 2)]
    across = across + [(b, a) for a, b in across]

    def exchange(x):
        return lax.ppermute(x, "rows", within), lax.ppermute(x, "rows", across)

    arrays = (shifts, stiffness, mass, factor)
    mine, shift_rows = pl.pallas_call(
        pack_kernel,
        in_specs=[pl.BlockSpec(memory_space=pltpu.HBM)] * 4,
        out_specs=[vmem(), vmem()],
        out_shape=[
            jax.ShapeDtypeStruct((CELLS, block + 2 * entries * rows, LANES), f32),
            jax.ShapeDtypeStruct((steps, 8, LANES), f32),
        ],
        scratch_shapes=[pltpu.VMEM((width, LANES), f32), pltpu.VMEM((LANES, width), f32)]
        + [pltpu.SMEM(shifts.shape, f32)]
        + [pltpu.VMEM(array.shape, f32) for array in arrays[1:]]
        + [pltpu.SemaphoreType.DMA] * 4,
        compiler_params=params(),
        name="pack",
    )(*arrays)

    z_shape = (ITERS, CELLS + 2, (rows + 2) * cols, LANES)
    coef_shape = (2, entries, CELLS, ext_pad, LANES)
    factor_shapes = (
        (entries, CELLS, ext_pad, LANES),
        (PLANES, ext_pad, LANES),
        (3, CHUNK_PLANES, SUB, LANES),
    )
    work = [(CELLS - 1, ext * cols, LANES), (ext * cols, LANES)]
    low_spec = pl.BlockSpec(memory_space=pl.ANY)
    coefs = None
    lowrank = None
    factors = ()
    for step in range(steps):
        first = step == 0
        last = step + 1 == steps
        even, odd = exchange(mine)
        if not first:
            outs = pl.pallas_call(
                functools.partial(side_kernel, step=step - 1, rows=rows, cols=cols),
                grid=(1,),
                in_specs=[vmem()] * 4 + ([] if lowrank is None else [low_spec]),
                out_specs=[low_block(steps, rows, cols, width, step - 1)] + [vmem()] * 4,
                out_shape=[
                    jax.ShapeDtypeStruct(shape, f32)
                    for shape in ((steps, rows, cols, width),) + factor_shapes + ((CELLS + 2, block, LANES),)
                ],
                scratch_shapes=[
                    pltpu.VMEM((CELLS - 1, block, LANES), f32),
                    pltpu.VMEM((block, LANES), f32),
                    pltpu.VMEM((width, LANES), f32),
                ],
                input_output_aliases={} if lowrank is None else {4: 0},
                compiler_params=params(),
                name=f"side{step}",
            )(*((shift_rows, coefs, mine, u_mine) + (() if lowrank is None else (lowrank,))))
            lowrank = outs[0]
            factors = tuple(outs[1:])
        shapes = [z_shape, (peers, gram_rows, LANES)]
        if first:
            shapes = [coef_shape] + shapes
        scratch = [(ITERS + 1, CELLS, ext * cols, LANES), (CELLS + 2, ext * cols, LANES)] + work
        scratch = scratch + [(gram_rows * LANES, LANES)] + (list(factor_shapes) if first else [])
        outs = pl.pallas_call(
            functools.partial(krylov_kernel, step=step, first=first, rows=rows, cols=cols, peers=peers),
            in_specs=[smem()] + [vmem()] * (4 + len(factors)),
            out_specs=[vmem() for shape in shapes],
            out_shape=[jax.ShapeDtypeStruct(shape, f32) for shape in shapes],
            scratch_shapes=[pltpu.VMEM(shape, f32) for shape in scratch],
            compiler_params=params(),
            name=f"krylov{step}",
        )(parity, shift_rows, mine, even, odd, *factors)
        if first:
            coefs = outs[0]
            outs = outs[1:]
        z, gram = outs
        gram = lax.all_to_all(gram, "rows", 0, 0)
        chunked = (CELLS, block, LANES)
        shapes = [(steps, rows, cols, width), (rows, cols, width)] if last else [chunked, chunked]
        alias = last and lowrank is not None
        u_mine, mine = pl.pallas_call(
            functools.partial(update_kernel, step=step, last=last, rows=rows, cols=cols),
            grid=(1,),
            in_specs=[vmem()] * 5 + ([low_spec] if alias else []),
            out_specs=[low_block(steps, rows, cols, width, step) if last else vmem(), vmem()],
            out_shape=[jax.ShapeDtypeStruct(shape, f32) for shape in shapes],
            scratch_shapes=[
                pltpu.VMEM((CELLS + 2, (rows + 2) * cols, LANES), f32),
                pltpu.VMEM((ITERS, cols, LANES), f32),
                pltpu.VMEM(chunked, f32),
                pltpu.VMEM((width, LANES), f32),
            ],
            input_output_aliases={5: 0} if alias else {},
            compiler_params=params(),
            name=f"update{step}",
        )(*((shift_rows, gram, z, mine, coefs) + ((lowrank,) if alias else ())))
    return u_mine, mine


def solution(mesh):
    in_specs = (P(None, "rows", None), P(None, "rows", None), P(), P("rows", None, None))
    out_specs = (P(None, "rows", None, None), P("rows", None, None))
    return jax.shard_map(shards, mesh=mesh, in_specs=in_specs, out_specs=out_specs, check_vma=False)
```

```python
import functools

import jax
import jax.numpy as jnp
from jax import lax
from jax.experimental import pallas as pl
from jax.experimental.pallas import tpu as pltpu
from jax.sharding import PartitionSpec as P


ITERS = 4
CELLS = 4
LANES = 128
PIVOT_TOL = 3e-7
OFFSETS = ((-1, -1), (-1, 0), (-1, 1), (0, -1), (0, 0), (0, 1), (1, -1), (1, 0), (1, 1))
OFF_ROW = (0, 1, 2, 6, 7, 8)
PAIRS = [(i, j) for i in range(ITERS + 1) for j in range(i, ITERS + 1)]

SUB = 8
DEPTH = LANES // SUB

E1, E2, G0, G1, G2, C0, C1, A3, L0, L1, L2, R0, R1, R2 = range(14)
PLANES = 14
TE, TINV, TH, TL, TR, TC3, TL0N, TR0N = range(8)
SINGLE = 8 * DEPTH
SA, SC, SB1, SF1, SB2, SF2, S4, SINV = range(8)
CHUNK_PLANES = SINGLE + 8


def roll(x, shift, axis=0):
    return pltpu.roll(x, shift % x.shape[axis], axis)


def params():
    return pltpu.CompilerParams(vmem_limit_bytes=40 * 1024 * 1024)


def to_chunks(natural, stage):
    for tile in range(CELLS):
        stage[tile * LANES : (tile + 1) * LANES, :] = natural[:, tile * LANES : (tile + 1) * LANES].T
    return [
        jnp.concatenate(
            [stage[pl.ds(depth * CELLS + cell, SUB, stride=CELLS * DEPTH), :] for depth in range(DEPTH)], axis=0
        ).T
        for cell in range(CELLS)
    ]


def from_chunks(planes, stage):
    for cell in range(CELLS):
        turned = planes[cell].T
        for depth in range(DEPTH):
            stage[pl.ds(depth * CELLS + cell, SUB, stride=CELLS * DEPTH), :] = turned[
                depth * SUB : (depth + 1) * SUB, :
            ]
    return [stage[tile * LANES : (tile + 1) * LANES, :].T for tile in range(CELLS)]


def split(matrix):
    return [matrix[depth * SUB : (depth + 1) * SUB, :] for depth in range(DEPTH)]


def next_chunk(registers):
    return registers[1:] + [roll(registers[0], -1)]


def previous_chunk(registers):
    return [roll(registers[-1], 1)] + registers[:-1]


def pack_kernel(
    shift_hbm, stiff_hbm, mass_hbm, factor_hbm, coefs_out, field_out, shifts_out,
    stage, gather, shift_ref, stiff_ref, mass_ref, factor_ref, shift_sem, stiff_sem, mass_sem, factor_sem,
):
    copies = [
        pltpu.make_async_copy(*operands)
        for operands in (
            (factor_hbm, factor_ref, factor_sem),
            (stiff_hbm, stiff_ref, stiff_sem),
            (mass_hbm, mass_ref, mass_sem),
            (shift_hbm, shift_ref, shift_sem),
        )
    ]
    for copy in copies:
        copy.start()
    rows, cols, width = factor_ref.shape
    entries = len(OFFSETS)
    gather[...] = jnp.zeros(gather.shape, jnp.float32)
    for which, ref in enumerate((stiff_ref, mass_ref)):
        copies[1 + which].wait()
        for entry in range(entries):
            at = (which * entries + entry) * rows
            gather[at : at + rows, :] = ref[entry]
    planes = to_chunks(gather[...], stage)
    count = 2 * entries * rows
    lane = lax.broadcasted_iota(jnp.int32, (count, LANES), 1)
    line = lax.broadcasted_iota(jnp.int32, (count, LANES), 0)
    column = (line // rows) % 3
    for cell in range(CELLS):
        plane = planes[cell][0:count, :]
        if cell == 0:
            plane = jnp.where((lane == 0) & (column == 0), 0.0, plane)
        if cell == CELLS - 1:
            plane = jnp.where((lane == LANES - 1) & (column == 2), 0.0, plane)
        coefs_out[cell] = plane
    copies[0].wait()
    planes = to_chunks(factor_ref[...].reshape(rows * cols, width), stage)
    for cell in range(CELLS):
        field_out[cell] = planes[cell]
    copies[3].wait()
    for step in range(shifts_out.shape[0]):
        shifts_out[step] = jnp.full(shifts_out.shape[1:], shift_ref[step], jnp.float32)


def factor_chunks(group, below, center, above, c3, l0, r0, chunk):
    l0n, r0n = next_chunk(l0), next_chunk(r0)
    center = [center[v] + c3[v] * l0n[v] for v in range(DEPTH)]
    above = [c3[v] * r0n[v] for v in range(DEPTH)]

    def put(index, value):
        chunk[group, index] = value

    for v in range(DEPTH):
        put(TC3 * DEPTH + v, c3[v])
        put(TL0N * DEPTH + v, l0n[v])
        put(TR0N * DEPTH + v, r0n[v])
    last = DEPTH - 1
    inv, hi, left = [], [], []
    for v in range(last):
        if v == 0:
            inv.append(1.0 / center[0])
            left.append(-below[0])
        else:
            e = below[v] * inv[v - 1]
            put(TE * DEPTH + v, e)
            inv.append(1.0 / (center[v] - e * above[v - 1]))
            left.append(-e * left[v - 1])
        hi.append(above[v] * inv[v])
        put(TINV * DEPTH + v, inv[v])
        put(TH * DEPTH + v, hi[v])
    l = [None] * last
    r = [None] * last
    for v in reversed(range(last)):
        l[v] = left[v] * inv[v]
        if v == last - 1:
            r[v] = -hi[v]
        else:
            l[v] = l[v] - hi[v] * l[v + 1]
            r[v] = -hi[v] * r[v + 1]
        put(TL * DEPTH + v, l[v])
        put(TR * DEPTH + v, r[v])
    put(SINGLE + SA, below[last])
    put(SINGLE + SC, above[last])
    b = below[last] * l[last - 1]
    d = center[last] + below[last] * r[last - 1] + above[last] * roll(l[0], -1)
    f = above[last] * roll(r[0], -1)
    slot = SB1
    stride = 1
    while stride < SUB:
        inverse = 1.0 / d
        from_below = -b * roll(inverse, stride)
        from_above = -f * roll(inverse, -stride)
        d = d + from_below * roll(f, stride) + from_above * roll(b, -stride)
        b, f = from_below * roll(b, stride), from_above * roll(f, -stride)
        if 2 * stride == SUB:
            put(SINGLE + S4, from_below + from_above)
        else:
            put(SINGLE + slot, from_below)
            put(SINGLE + slot + 1, from_above)
            slot += 2
        stride *= 2
    put(SINGLE + SINV, 1.0 / d)


def solve_chunks(group, q, p0, chunk):
    def get(index):
        return chunk[group, index]

    p0n = next_chunk(p0)
    q = [q[v] - get(TC3 * DEPTH + v) * p0n[v] for v in range(DEPTH)]
    last = DEPTH - 1
    f = [q[0]]
    for v in range(1, last):
        f.append(q[v] - get(TE * DEPTH + v) * f[v - 1])
    p = [None] * last
    for v in reversed(range(last)):
        p[v] = f[v] * get(TINV * DEPTH + v)
        if v < last - 1:
            p[v] = p[v] - get(TH * DEPTH + v) * p[v + 1]
    s = q[last] - get(SINGLE + SA) * p[last - 1] - get(SINGLE + SC) * roll(p[0], -1)
    s = s + get(SINGLE + SB1) * roll(s, 1) + get(SINGLE + SF1) * roll(s, -1)
    s = s + get(SINGLE + SB2) * roll(s, 2) + get(SINGLE + SF2) * roll(s, -2)
    s = s + get(SINGLE + S4) * roll(s, 4)
    s = s * get(SINGLE + SINV)
    before = roll(s, 1)
    x = [p[v] + get(TL * DEPTH + v) * before + get(TR * DEPTH + v) * s for v in range(last)] + [s]
    xn = next_chunk(x)
    x0n = [p0n[v] + get(TL0N * DEPTH + v) * x[v] + get(TR0N * DEPTH + v) * xn[v] for v in range(DEPTH)]
    return x, previous_chunk(x), x0n


def build_lines(coefs_ref, shift, line, ext):
    for entry in range(len(OFFSETS)):
        for cell in range(CELLS):
            line[entry, cell, 0:ext, :] = (
                coefs_ref[0, entry, cell, 0:ext, :] + shift * coefs_ref[1, entry, cell, 0:ext, :]
            )


def build_factors(line, inner, chunk, rows, cols, ext):
    a = [line[3, cell, 0:ext, :] for cell in range(CELLS)]
    d = [line[4, cell, 0:ext, :] for cell in range(CELLS)]
    c = [line[5, cell, 0:ext, :] for cell in range(CELLS)]
    d = [jnp.where(x <= 0.0, 1.0, x) for x in d]
    g0 = 1.0 / d[0]
    e1 = a[1] * g0
    g1 = 1.0 / (d[1] - e1 * c[0])
    e2 = a[2] * g1
    g2 = 1.0 / (d[2] - e2 * c[1])
    f0 = -a[0]
    f1 = -e1 * f0
    f2 = -e2 * f1
    l2 = f2 * g2
    l1 = (f1 - c[1] * l2) * g1
    l0 = (f0 - c[0] * l1) * g0
    r2 = -c[2] * g2
    r1 = -c[1] * r2 * g1
    r0 = -c[0] * r1 * g0
    for index, value in (
        (E1, e1), (E2, e2), (G0, g0), (G1, g1), (G2, g2), (C0, c[0]), (C1, c[1]), (A3, a[3]),
        (L0, l0), (L1, l1), (L2, l2), (R0, r0), (R1, r1), (R2, r2),
    ):
        inner[index, 0:ext, :] = value
    planes = (a[3] * l2, d[3] + a[3] * r2, c[3], l0, r0)
    for group in range(ext // rows):
        turned = [
            split(
                jnp.concatenate(
                    [
                        jnp.broadcast_to(plane[row : row + 1, :], (cols, LANES))
                        for row in range(group * rows, (group + 1) * rows)
                    ],
                    axis=0,
                ).T
            )
            for plane in planes
        ]
        below, center, c3, l0t, r0t = turned
        factor_chunks(group, below, center, None, c3, l0t, r0t, chunk)


def stencil_rows(coef, entries, read, row):
    out = []
    for cell in range(CELLS):
        total = None
        for entry in entries:
            offset = OFFSETS[entry]
            term = coef(entry, cell) * read(1 + cell + offset[1], row + offset[0])
            total = term if total is None else total + term
        out.append(total)
    return out


def line_solve(group, wanted, read, inner, chunk, px, qx, zx, base, rows, cols):
    def coef(index, row):
        return inner[index, row : row + 1, :]

    def span(row, count=1):
        return slice((row - base) * cols, (row - base + count) * cols)

    for row in wanted:
        v0, v1, v2, v3 = (read(cell, row) for cell in range(CELLS))
        f1 = v1 - coef(E1, row) * v0
        f2 = v2 - coef(E2, row) * f1
        x2 = f2 * coef(G2, row)
        x1 = (f1 - coef(C1, row) * x2) * coef(G1, row)
        x0 = (v0 - coef(C0, row) * x1) * coef(G0, row)
        px[0, span(row), :] = x0
        px[1, span(row), :] = x1
        px[2, span(row), :] = x2
        qx[span(row), :] = v3 - coef(A3, row) * x2
    at = span(group * rows, rows)
    x, before, after = solve_chunks(group, split(qx[at, :].T), split(px[0, at, :].T), chunk)
    zx[CELLS, at, :] = jnp.concatenate(x, axis=0).T
    zx[0, at, :] = jnp.concatenate(before, axis=0).T
    zx[CELLS + 1, at, :] = jnp.concatenate(after, axis=0).T
    for row in wanted:
        x3 = zx[CELLS, span(row), :]
        x3b = zx[0, span(row), :]
        for cell in range(CELLS - 1):
            zx[1 + cell, span(row), :] = (
                px[cell, span(row), :] + coef(L0 + cell, row) * x3b + coef(R0 + cell, row) * x3
            )


def side_kernel(parity_ref, shift_ref, *refs, step, rows, cols):
    ext = 3 * rows
    entries = len(OFFSETS)
    if step == 0:
        own_ref, even_ref, odd_ref, mine_ref, coefs_ref, line, inner, chunk, z_out, px, qx = refs
        low_is_even = parity_ref[0] == 1
        for which in range(2):
            for entry in range(entries):
                at = (which * entries + entry) * rows
                for cell in range(CELLS):
                    even = even_ref[cell, at : at + rows, :]
                    odd = odd_ref[cell, at : at + rows, :]
                    coefs_ref[which, entry, cell, 0:rows, :] = jnp.where(low_is_even, even, odd)
                    coefs_ref[which, entry, cell, rows : 2 * rows, :] = own_ref[cell, at : at + rows, :]
                    coefs_ref[which, entry, cell, 2 * rows : ext, :] = jnp.where(low_is_even, odd, even)
    else:
        coefs_ref, mine_ref, u_ref = refs[:3]
        low_out, line, inner, chunk, z_out, px, qx, stage = refs[-8:]
    build_lines(coefs_ref, shift_ref[step, 0:1, :], line, ext)
    build_factors(line, inner, chunk, rows, cols, ext)

    def read(cell, row):
        return mine_ref[cell, (row - rows) * cols : (row - rows + 1) * cols, :]

    line_solve(1, list(range(rows, 2 * rows)), read, inner, chunk, px, qx, z_out, rows, rows, cols)
    if step > 0:
        root = jnp.sqrt(2.0 * shift_ref[step - 1, 0:1, :])
        write_natural(low_out, 0, [root * u_ref[cell] for cell in range(CELLS)], stage, rows, cols)


def write_natural(out, lead, planes, stage, rows, cols):
    tiles = from_chunks(planes, stage)
    for tile in range(len(tiles)):
        value = tiles[tile].reshape(rows, cols, LANES)
        if lead is None:
            out[:, :, tile * LANES : (tile + 1) * LANES] = value
        else:
            out[lead, :, :, tile * LANES : (tile + 1) * LANES] = value


def krylov_kernel(
    parity_ref, mine_ref, even_ref, odd_ref, line, inner, chunk, z_mine,
    z_out, gram_out, wx, zx, px, qx, sums, *, rows, cols, peers,
):
    ext = 3 * rows
    block = rows * cols
    parity = parity_ref[0]
    at_even = jnp.where(parity == 0, 2 * rows, 0)
    at_odd = 2 * rows - at_even
    wx[0, :, pl.ds(rows * cols, block), :] = mine_ref[...]
    wx[0, :, pl.ds(pl.multiple_of(at_even * cols, cols), block), :] = even_ref[...]
    wx[0, :, pl.ds(pl.multiple_of(at_odd * cols, cols), block), :] = odd_ref[...]

    def span(row, count=1):
        return slice(row * cols, (row + count) * cols)

    for k in range(ITERS):
        low, high = k, ext - k

        def read_w(cell, row):
            return wx[k, cell, span(row), :]

        for group in range(ext // rows):
            if k == 0 and group == 1:
                zx[:, span(rows, rows), :] = z_mine[...]
                continue
            wanted = [row for row in range(group * rows, (group + 1) * rows) if low <= row < high]
            line_solve(group, wanted, read_w, inner, chunk, px, qx, zx, 0, rows, cols)
        for row in range(rows - 1, 2 * rows + 1):
            z_out[k, :, span(row - rows + 1), :] = zx[:, span(row), :]

        def read_z(slot, row):
            return zx[slot, span(row), :]

        for row in range(low + 1, high - 1):
            image = stencil_rows(lambda entry, cell: line[entry, cell, row : row + 1, :], OFF_ROW, read_z, row)
            for cell in range(CELLS):
                wx[k + 1, cell, span(row), :] = image[cell]

    for tile in range(cols // 8):
        total = [None] * len(PAIRS)
        for row in range(rows, 2 * rows):
            for cell in range(CELLS):
                at = row * cols + tile * 8
                w = [wx[k, cell, at : at + 8, :] for k in range(ITERS + 1)]
                for index, (i, j) in enumerate(PAIRS):
                    term = w[i] * w[j]
                    total[index] = term if total[index] is None else total[index] + term
        for index in range(len(PAIRS)):
            sums[index * cols + tile * 8 : index * cols + tile * 8 + 8, :] = total[index]
    sums[len(PAIRS) * cols :, :] = jnp.zeros((sums.shape[0] - len(PAIRS) * cols, LANES), jnp.float32)
    for part in range(sums.shape[0] // LANES):
        turned = sums[part * LANES : (part + 1) * LANES, :].T
        gram_out[:, part : part + 1, :] = jnp.broadcast_to(
            jnp.sum(turned, axis=0, keepdims=True)[None], (peers, 1, LANES)
        )


def weights_of(g):
    upper = [
        [(g[i, j] + g[i + 1, j + 1]) + (g[i, j + 1] + g[i + 1, j]) for j in range(ITERS)] for i in range(ITERS)
    ]
    diag = [upper[i][i] for i in range(ITERS)]
    right = [g[0, i] + g[0, i + 1] for i in range(ITERS)]
    inverse = [None] * ITERS
    for k in range(ITERS):
        good = upper[k][k] > PIVOT_TOL * diag[k]
        inverse[k] = jnp.where(good, 1.0 / jnp.where(good, upper[k][k], 1.0), 0.0)
        for i in range(k + 1, ITERS):
            scale = upper[k][i] * inverse[k]
            for j in range(i, ITERS):
                upper[i][j] = upper[i][j] - scale * upper[k][j]
            right[i] = right[i] - scale * right[k]
    y = [None] * ITERS
    for k in reversed(range(ITERS)):
        value = right[k]
        for j in range(k + 1, ITERS):
            value = value - upper[k][j] * y[j]
        y[k] = value * inverse[k]
    return y


def update_kernel(shift_ref, gram_ref, z_ref, mine_ref, coefs_ref, *refs, step, last, rows, cols):
    low_out, next_out, ux, yx, own, stage = refs[-6:]
    parts = [gram_ref[peer] for peer in range(gram_ref.shape[0])]
    while len(parts) > 1:
        parts = [a + b for a, b in zip(parts[0::2], parts[1::2])] + parts[len(parts) // 2 * 2 :]
    total = parts[0]
    g = {}
    per_part = LANES // cols
    for part in range(total.shape[0]):
        turned = jnp.broadcast_to(total[part : part + 1, :], (LANES, LANES)).T
        for index, (i, j) in enumerate(PAIRS[part * per_part : (part + 1) * per_part]):
            g[i, j] = g[j, i] = turned[index * cols : (index + 1) * cols, :]
    y = weights_of(g)
    for k in range(ITERS):
        yx[k] = y[k]

    def span(row, count=1):
        return slice(row * cols, (row + count) * cols)

    for row in range(rows + 2):
        for slot in range(CELLS + 2):
            value = yx[0] * z_ref[0, slot, span(row), :]
            for k in range(1, ITERS):
                value = value + yx[k] * z_ref[k, slot, span(row), :]
            ux[slot, span(row), :] = value
            if not last and 0 < row <= rows and 0 < slot <= CELLS:
                low_out[slot - 1, span(row - 1), :] = value

    def read_u(slot, row):
        return ux[slot, span(row), :]

    double = 2.0 * shift_ref[step, 0:1, :]
    for row in range(rows):
        image = stencil_rows(
            lambda entry, cell: coefs_ref[1, entry, cell, rows + row : rows + row + 1, :],
            range(len(OFFSETS)), read_u, row + 1,
        )
        for cell in range(CELLS):
            value = mine_ref[cell, span(row), :] - double * image[cell]
            if last:
                own[cell, span(row), :] = value
            else:
                next_out[cell, span(row), :] = value
    if last:
        root = jnp.sqrt(double)
        planes = [root * ux[1 + cell, span(1, rows), :] for cell in range(CELLS)]
        write_natural(low_out, 0, planes, stage, rows, cols)
        write_natural(next_out, None, [own[cell] for cell in range(CELLS)], stage, rows, cols)


def vmem():
    return pl.BlockSpec(memory_space=pltpu.VMEM)


def low_block(rows, cols, width, step):
    return pl.BlockSpec((1, rows, cols, width), lambda i: (step, 0, 0, 0))


def smem():
    return pl.BlockSpec(memory_space=pltpu.SMEM)


def shards(stiffness, mass, shifts, factor):
    rows, cols, width = factor.shape
    steps = shifts.shape[0]
    entries = len(OFFSETS)
    peers = lax.axis_size("rows")
    parity = (lax.axis_index("rows") % 2).astype(jnp.int32).reshape(1)
    block = rows * cols
    ext = 3 * rows
    ext_pad = -(-ext // 8) * 8
    f32 = jnp.float32
    gram_rows = -(-len(PAIRS) * cols // LANES)
    assert block == LANES and width == CELLS * LANES

    within = [(i, i ^ 1) for i in range(peers) if i ^ 1 < peers]
    across = [(i, i + 1) for i in range(1, peers - 1, 2)]
    across = across + [(b, a) for a, b in across]

    def exchange(x):
        return lax.ppermute(x, "rows", within), lax.ppermute(x, "rows", across)

    arrays = [
        pltpu.with_memory_space_constraint(array, pltpu.HBM) for array in (shifts, stiffness, mass, factor)
    ]
    chunked = (CELLS, block, LANES)
    stencils, mine, shift_rows = pl.pallas_call(
        pack_kernel,
        in_specs=[pl.BlockSpec(memory_space=pltpu.HBM)] * 4,
        out_specs=[vmem()] * 3,
        out_shape=[
            jax.ShapeDtypeStruct(shape, f32)
            for shape in ((CELLS, 2 * entries * rows, LANES), chunked, (steps, 8, LANES))
        ],
        scratch_shapes=[pltpu.VMEM((width, LANES), f32), pltpu.VMEM((LANES, width), f32)]
        + [pltpu.SMEM(shifts.shape, f32)]
        + [pltpu.VMEM(array.shape, f32) for array in (stiffness, mass, factor)]
        + [pltpu.SemaphoreType.DMA] * 4,
        compiler_params=params(),
        name="pack",
    )(*arrays)

    z_shape = (ITERS, CELLS + 2, (rows + 2) * cols, LANES)
    coef_shape = (2, entries, CELLS, ext_pad, LANES)
    factor_shapes = (
        (entries, CELLS, ext_pad, LANES),
        (PLANES, ext_pad, LANES),
        (3, CHUNK_PLANES, SUB, LANES),
        (CELLS + 2, block, LANES),
    )
    low_shape = (steps, rows, cols, width)
    low_spec = pl.BlockSpec(memory_space=pl.ANY)
    coefs = None
    lowrank = None
    for step in range(steps):
        first = step == 0
        last = step + 1 == steps
        if first:
            beside = (stencils, *exchange(stencils), mine)
            lead_shape, lead_spec = coef_shape, vmem()
            scratch = []
        else:
            beside = (coefs, mine, u_mine) + (() if lowrank is None else (lowrank,))
            lead_shape, lead_spec = low_shape, low_block(rows, cols, width, step - 1)
            scratch = [pltpu.VMEM((width, LANES), f32)]
        even, odd = exchange(mine)
        lead, *factors = pl.pallas_call(
            functools.partial(side_kernel, step=step, rows=rows, cols=cols),
            grid=(1,),
            in_specs=[smem()] + [vmem()] * (5 if first else 4) + [low_spec] * (len(beside) - (4 if first else 3)),
            out_specs=[lead_spec] + [vmem()] * 4,
            out_shape=[jax.ShapeDtypeStruct(shape, f32) for shape in (lead_shape,) + factor_shapes],
            scratch_shapes=[pltpu.VMEM((CELLS - 1, block, LANES), f32), pltpu.VMEM((block, LANES), f32)] + scratch,
            input_output_aliases={} if first or lowrank is None else {5: 0},
            compiler_params=params(),
        )(parity, shift_rows, *beside)
        if first:
            coefs = lead
        else:
            lowrank = lead
        shapes = [z_shape, (peers, gram_rows, LANES)]
        scratch = [
            (ITERS + 1, CELLS, ext * cols, LANES),
            (CELLS + 2, ext * cols, LANES),
            (CELLS - 1, ext * cols, LANES),
            (ext * cols, LANES),
            (gram_rows * LANES, LANES),
        ]
        z, gram = pl.pallas_call(
            functools.partial(krylov_kernel, rows=rows, cols=cols, peers=peers),
            in_specs=[smem()] + [vmem()] * 7,
            out_specs=[vmem() for shape in shapes],
            out_shape=[jax.ShapeDtypeStruct(shape, f32) for shape in shapes],
            scratch_shapes=[pltpu.VMEM(shape, f32) for shape in scratch],
            compiler_params=params(),
            name="krylov",
        )(parity, mine, even, odd, *factors)
        gram = lax.all_to_all(gram, "rows", 0, 0)
        shapes = [low_shape, (rows, cols, width)] if last else [chunked, chunked]
        alias = last and lowrank is not None
        u_mine, mine = pl.pallas_call(
            functools.partial(update_kernel, step=step, last=last, rows=rows, cols=cols),
            grid=(1,),
            in_specs=[vmem()] * 5 + ([low_spec] if alias else []),
            out_specs=[low_block(rows, cols, width, step) if last else vmem(), vmem()],
            out_shape=[jax.ShapeDtypeStruct(shape, f32) for shape in shapes],
            scratch_shapes=[
                pltpu.VMEM((CELLS + 2, (rows + 2) * cols, LANES), f32),
                pltpu.VMEM((ITERS, cols, LANES), f32),
                pltpu.VMEM(chunked, f32),
                pltpu.VMEM((width, LANES), f32),
            ],
            input_output_aliases={5: 0} if alias else {},
            compiler_params=params(),
        )(*((shift_rows, gram, z, mine, coefs) + ((lowrank,) if alias else ())))
    return u_mine, mine


def solution(mesh):
    in_specs = (P(None, "rows", None), P(None, "rows", None), P(), P("rows", None, None))
    out_specs = (P(None, "rows", None, None), P("rows", None, None))
    return jax.shard_map(shards, mesh=mesh, in_specs=in_specs, out_specs=out_specs, check_vma=False)
```

```python
import functools

import jax
import jax.numpy as jnp
from jax import lax
from jax.experimental import pallas as pl
from jax.experimental.pallas import tpu as pltpu
from jax.sharding import PartitionSpec as P

ITERS = 4
CELLS = 4
LANES = 128
PIVOT_TOL = 3e-7
OFFSETS = ((-1, -1), (-1, 0), (-1, 1), (0, -1), (0, 0), (0, 1), (1, -1), (1, 0), (1, 1))
OFF_ROW = (0, 1, 2, 6, 7, 8)
PAIRS = [(i, j) for i in range(ITERS + 1) for j in range(i, ITERS + 1)]

SUB = 8
DEPTH = LANES // SUB

E1, E2, G0, G1, G2, C0, C1, A3, L0, L1, L2, R0, R1, R2 = range(14)
PLANES = 14
TE, TINV, TH, TL, TR, TC3, TL0N, TR0N = range(8)
SINGLE = 8 * DEPTH
SA, SC, SB1, SF1, SB2, SF2, S4, SINV = range(8)
CHUNK_PLANES = SINGLE + 8


def roll(x, shift, axis=0):
    return pltpu.roll(x, shift % x.shape[axis], axis)


def params():
    return pltpu.CompilerParams(vmem_limit_bytes=40 * 1024 * 1024)


def to_chunks(natural, stage):
    for tile in range(CELLS):
        stage[tile * LANES : (tile + 1) * LANES, :] = natural[:, tile * LANES : (tile + 1) * LANES].T
    return [
        jnp.concatenate(
            [stage[pl.ds(depth * CELLS + cell, SUB, stride=CELLS * DEPTH), :] for depth in range(DEPTH)], axis=0
        ).T
        for cell in range(CELLS)
    ]


def from_chunks(planes, stage):
    for cell in range(CELLS):
        turned = planes[cell].T
        for depth in range(DEPTH):
            stage[pl.ds(depth * CELLS + cell, SUB, stride=CELLS * DEPTH), :] = turned[
                depth * SUB : (depth + 1) * SUB, :
            ]
    return [stage[tile * LANES : (tile + 1) * LANES, :].T for tile in range(CELLS)]


def split(matrix):
    return [matrix[depth * SUB : (depth + 1) * SUB, :] for depth in range(DEPTH)]


def next_chunk(registers):
    return registers[1:] + [roll(registers[0], -1)]


def previous_chunk(registers):
    return [roll(registers[-1], 1)] + registers[:-1]


def pack_kernel(
    shift_hbm, stiff_hbm, mass_hbm, factor_hbm, coefs_out, field_out, shifts_out,
    stage, gather, shift_ref, stiff_ref, mass_ref, factor_ref, shift_sem, stiff_sem, mass_sem, factor_sem,
):
    copies = [
        pltpu.make_async_copy(*operands)
        for operands in (
            (factor_hbm, factor_ref, factor_sem),
            (stiff_hbm, stiff_ref, stiff_sem),
            (mass_hbm, mass_ref, mass_sem),
            (shift_hbm, shift_ref, shift_sem),
        )
    ]
    for copy in copies:
        copy.start()
    rows, cols, width = factor_ref.shape
    entries = len(OFFSETS)
    gather[...] = jnp.zeros(gather.shape, jnp.float32)
    for which, ref in enumerate((stiff_ref, mass_ref)):
        copies[1 + which].wait()
        for entry in range(entries):
            at = (which * entries + entry) * rows
            gather[at : at + rows, :] = ref[entry]
    planes = to_chunks(gather[...], stage)
    count = 2 * entries * rows
    lane = lax.broadcasted_iota(jnp.int32, (count, LANES), 1)
    line = lax.broadcasted_iota(jnp.int32, (count, LANES), 0)
    column = (line // rows) % 3
    for cell in range(CELLS):
        plane = planes[cell][0:count, :]
        if cell == 0:
            plane = jnp.where((lane == 0) & (column == 0), 0.0, plane)
        if cell == CELLS - 1:
            plane = jnp.where((lane == LANES - 1) & (column == 2), 0.0, plane)
        coefs_out[cell] = plane
    copies[0].wait()
    planes = to_chunks(factor_ref[...].reshape(rows * cols, width), stage)
    for cell in range(CELLS):
        field_out[cell] = planes[cell]
    copies[3].wait()
    for step in range(shifts_out.shape[0]):
        shifts_out[step] = jnp.full(shifts_out.shape[1:], shift_ref[step], jnp.float32)


def factor_chunks(group, below, center, above, c3, l0, r0, chunk):
    l0n, r0n = next_chunk(l0), next_chunk(r0)
    center = [center[v] + c3[v] * l0n[v] for v in range(DEPTH)]
    above = [c3[v] * r0n[v] for v in range(DEPTH)]

    def put(index, value):
        chunk[group, index] = value

    for v in range(DEPTH):
        put(TC3 * DEPTH + v, c3[v])
        put(TL0N * DEPTH + v, l0n[v])
        put(TR0N * DEPTH + v, r0n[v])
    last = DEPTH - 1
    inv, hi, left = [], [], []
    for v in range(last):
        if v == 0:
            inv.append(1.0 / center[0])
            left.append(-below[0])
        else:
            e = below[v] * inv[v - 1]
            put(TE * DEPTH + v, e)
            inv.append(1.0 / (center[v] - e * above[v - 1]))
            left.append(-e * left[v - 1])
        hi.append(above[v] * inv[v])
        put(TINV * DEPTH + v, inv[v])
        put(TH * DEPTH + v, hi[v])
    l = [None] * last
    r = [None] * last
    for v in reversed(range(last)):
        l[v] = left[v] * inv[v]
        if v == last - 1:
            r[v] = -hi[v]
        else:
            l[v] = l[v] - hi[v] * l[v + 1]
            r[v] = -hi[v] * r[v + 1]
        put(TL * DEPTH + v, l[v])
        put(TR * DEPTH + v, r[v])
    put(SINGLE + SA, below[last])
    put(SINGLE + SC, above[last])
    b = below[last] * l[last - 1]
    d = center[last] + below[last] * r[last - 1] + above[last] * roll(l[0], -1)
    f = above[last] * roll(r[0], -1)
    slot = SB1
    stride = 1
    while stride < SUB:
        inverse = 1.0 / d
        from_below = -b * roll(inverse, stride)
        from_above = -f * roll(inverse, -stride)
        d = d + from_below * roll(f, stride) + from_above * roll(b, -stride)
        b, f = from_below * roll(b, stride), from_above * roll(f, -stride)
        if 2 * stride == SUB:
            put(SINGLE + S4, from_below + from_above)
        else:
            put(SINGLE + slot, from_below)
            put(SINGLE + slot + 1, from_above)
            slot += 2
        stride *= 2
    put(SINGLE + SINV, 1.0 / d)


def solve_chunks(group, q, p0, chunk):
    def get(index):
        return chunk[group, index]

    p0n = next_chunk(p0)
    q = [q[v] - get(TC3 * DEPTH + v) * p0n[v] for v in range(DEPTH)]
    last = DEPTH - 1
    f = [q[0]]
    for v in range(1, last):
        f.append(q[v] - get(TE * DEPTH + v) * f[v - 1])
    p = [None] * last
    for v in reversed(range(last)):
        p[v] = f[v] * get(TINV * DEPTH + v)
        if v < last - 1:
            p[v] = p[v] - get(TH * DEPTH + v) * p[v + 1]
    s = q[last] - get(SINGLE + SA) * p[last - 1] - get(SINGLE + SC) * roll(p[0], -1)
    s = s + get(SINGLE + SB1) * roll(s, 1) + get(SINGLE + SF1) * roll(s, -1)
    s = s + get(SINGLE + SB2) * roll(s, 2) + get(SINGLE + SF2) * roll(s, -2)
    s = s + get(SINGLE + S4) * roll(s, 4)
    s = s * get(SINGLE + SINV)
    before = roll(s, 1)
    x = [p[v] + get(TL * DEPTH + v) * before + get(TR * DEPTH + v) * s for v in range(last)] + [s]
    xn = next_chunk(x)
    x0n = [p0n[v] + get(TL0N * DEPTH + v) * x[v] + get(TR0N * DEPTH + v) * xn[v] for v in range(DEPTH)]
    return x, previous_chunk(x), x0n


def build_lines(coefs_ref, shift, line, ext):
    for entry in range(len(OFFSETS)):
        for cell in range(CELLS):
            line[entry, cell, 0:ext, :] = (
                coefs_ref[0, entry, cell, 0:ext, :] + shift * coefs_ref[1, entry, cell, 0:ext, :]
            )


def build_factors(line, inner, chunk, rows, cols, ext):
    a = [line[3, cell, 0:ext, :] for cell in range(CELLS)]
    d = [line[4, cell, 0:ext, :] for cell in range(CELLS)]
    c = [line[5, cell, 0:ext, :] for cell in range(CELLS)]
    d = [jnp.where(x <= 0.0, 1.0, x) for x in d]
    g0 = 1.0 / d[0]
    e1 = a[1] * g0
    g1 = 1.0 / (d[1] - e1 * c[0])
    e2 = a[2] * g1
    g2 = 1.0 / (d[2] - e2 * c[1])
    f0 = -a[0]
    f1 = -e1 * f0
    f2 = -e2 * f1
    l2 = f2 * g2
    l1 = (f1 - c[1] * l2) * g1
    l0 = (f0 - c[0] * l1) * g0
    r2 = -c[2] * g2
    r1 = -c[1] * r2 * g1
    r0 = -c[0] * r1 * g0
    for index, value in (
        (E1, e1), (E2, e2), (G0, g0), (G1, g1), (G2, g2), (C0, c[0]), (C1, c[1]), (A3, a[3]),
        (L0, l0), (L1, l1), (L2, l2), (R0, r0), (R1, r1), (R2, r2),
    ):
        inner[index, 0:ext, :] = value
    planes = (a[3] * l2, d[3] + a[3] * r2, c[3], l0, r0)
    for group in range(ext // rows):
        turned = [
            split(
                jnp.concatenate(
                    [
                        jnp.broadcast_to(plane[row : row + 1, :], (cols, LANES))
                        for row in range(group * rows, (group + 1) * rows)
                    ],
                    axis=0,
                ).T
            )
            for plane in planes
        ]
        below, center, c3, l0t, r0t = turned
        factor_chunks(group, below, center, None, c3, l0t, r0t, chunk)


def stencil_rows(coef, entries, read, row):
    out = []
    for cell in range(CELLS):
        total = None
        for entry in entries:
            offset = OFFSETS[entry]
            term = coef(entry, cell) * read(1 + cell + offset[1], row + offset[0])
            total = term if total is None else total + term
        out.append(total)
    return out


def line_solve(group, wanted, read, inner, chunk, px, qx, zx, base, rows, cols):
    def coef(index, row):
        return inner[index, row : row + 1, :]

    def span(row, count=1):
        return slice((row - base) * cols, (row - base + count) * cols)

    for row in wanted:
        v0, v1, v2, v3 = (read(cell, row) for cell in range(CELLS))
        f1 = v1 - coef(E1, row) * v0
        f2 = v2 - coef(E2, row) * f1
        x2 = f2 * coef(G2, row)
        x1 = (f1 - coef(C1, row) * x2) * coef(G1, row)
        x0 = (v0 - coef(C0, row) * x1) * coef(G0, row)
        px[0, span(row), :] = x0
        px[1, span(row), :] = x1
        px[2, span(row), :] = x2
        qx[span(row), :] = v3 - coef(A3, row) * x2
    at = span(group * rows, rows)
    x, before, after = solve_chunks(group, split(qx[at, :].T), split(px[0, at, :].T), chunk)
    zx[CELLS, at, :] = jnp.concatenate(x, axis=0).T
    zx[0, at, :] = jnp.concatenate(before, axis=0).T
    zx[CELLS + 1, at, :] = jnp.concatenate(after, axis=0).T
    for row in wanted:
        x3 = zx[CELLS, span(row), :]
        x3b = zx[0, span(row), :]
        for cell in range(CELLS - 1):
            zx[1 + cell, span(row), :] = (
                px[cell, span(row), :] + coef(L0 + cell, row) * x3b + coef(R0 + cell, row) * x3
            )


def side_kernel(parity_ref, shift_ref, *refs, step, rows, cols):
    ext = 3 * rows
    entries = len(OFFSETS)
    if step == 0:
        own_ref, even_ref, odd_ref, mine_ref, coefs_ref, line, inner, chunk, z_out, px, qx = refs
        low_is_even = parity_ref[0] == 1
        for which in range(2):
            for entry in range(entries):
                at = (which * entries + entry) * rows
                for cell in range(CELLS):
                    even = even_ref[cell, at : at + rows, :]
                    odd = odd_ref[cell, at : at + rows, :]
                    coefs_ref[which, entry, cell, 0:rows, :] = jnp.where(low_is_even, even, odd)
                    coefs_ref[which, entry, cell, rows : 2 * rows, :] = own_ref[cell, at : at + rows, :]
                    coefs_ref[which, entry, cell, 2 * rows : ext, :] = jnp.where(low_is_even, odd, even)
    else:
        coefs_ref, mine_ref, u_ref = refs[:3]
        low_out, line, inner, chunk, z_out, px, qx, stage = refs[-8:]
    build_lines(coefs_ref, shift_ref[step, 0:1, :], line, ext)
    build_factors(line, inner, chunk, rows, cols, ext)

    def read(cell, row):
        return mine_ref[cell, (row - rows) * cols : (row - rows + 1) * cols, :]

    line_solve(1, list(range(rows, 2 * rows)), read, inner, chunk, px, qx, z_out, rows, rows, cols)
    if step > 0:
        root = jnp.sqrt(2.0 * shift_ref[step - 1, 0:1, :])
        write_natural(low_out, 0, [root * u_ref[cell] for cell in range(CELLS)], stage, rows, cols)


def write_natural(out, lead, planes, stage, rows, cols):
    tiles = from_chunks(planes, stage)
    for tile in range(len(tiles)):
        value = tiles[tile].reshape(rows, cols, LANES)
        if lead is None:
            out[:, :, tile * LANES : (tile + 1) * LANES] = value
        else:
            out[lead, :, :, tile * LANES : (tile + 1) * LANES] = value


def krylov_kernel(
    parity_ref, mine_ref, even_ref, odd_ref, line, inner, chunk, z_mine,
    z_out, gram_out, wx, zx, px, qx, sums, *, rows, cols, peers,
):
    ext = 3 * rows
    block = rows * cols
    parity = parity_ref[0]
    at_even = jnp.where(parity == 0, 2 * rows, 0)
    at_odd = 2 * rows - at_even
    wx[0, :, pl.ds(rows * cols, block), :] = mine_ref[...]
    wx[0, :, pl.ds(pl.multiple_of(at_even * cols, cols), block), :] = even_ref[...]
    wx[0, :, pl.ds(pl.multiple_of(at_odd * cols, cols), block), :] = odd_ref[...]

    def span(row, count=1):
        return slice(row * cols, (row + count) * cols)

    for k in range(ITERS):
        low, high = k, ext - k

        def read_w(cell, row):
            return wx[k, cell, span(row), :]

        for group in range(ext // rows):
            if k == 0 and group == 1:
                zx[:, span(rows, rows), :] = z_mine[...]
                continue
            wanted = [row for row in range(group * rows, (group + 1) * rows) if low <= row < high]
            line_solve(group, wanted, read_w, inner, chunk, px, qx, zx, 0, rows, cols)
        for row in range(rows - 1, 2 * rows + 1):
            z_out[k, :, span(row - rows + 1), :] = zx[:, span(row), :]

        def read_z(slot, row):
            return zx[slot, span(row), :]

        for row in range(low + 1, high - 1):
            image = stencil_rows(lambda entry, cell: line[entry, cell, row : row + 1, :], OFF_ROW, read_z, row)
            for cell in range(CELLS):
                wx[k + 1, cell, span(row), :] = image[cell]

    for tile in range(cols // 8):
        total = [None] * len(PAIRS)
        for row in range(rows, 2 * rows):
            for cell in range(CELLS):
                at = row * cols + tile * 8
                w = [wx[k, cell, at : at + 8, :] for k in range(ITERS + 1)]
                for index, (i, j) in enumerate(PAIRS):
                    term = w[i] * w[j]
                    total[index] = term if total[index] is None else total[index] + term
        for index in range(len(PAIRS)):
            sums[index * cols + tile * 8 : index * cols + tile * 8 + 8, :] = total[index]
    sums[len(PAIRS) * cols :, :] = jnp.zeros((sums.shape[0] - len(PAIRS) * cols, LANES), jnp.float32)
    for part in range(sums.shape[0] // LANES):
        turned = sums[part * LANES : (part + 1) * LANES, :].T
        gram_out[:, part : part + 1, :] = jnp.broadcast_to(
            jnp.sum(turned, axis=0, keepdims=True)[None], (peers, 1, LANES)
        )


def weights_of(g):
    upper = [
        [(g[i, j] + g[i + 1, j + 1]) + (g[i, j + 1] + g[i + 1, j]) for j in range(ITERS)] for i in range(ITERS)
    ]
    diag = [upper[i][i] for i in range(ITERS)]
    right = [g[0, i] + g[0, i + 1] for i in range(ITERS)]
    inverse = [None] * ITERS
    for k in range(ITERS):
        good = upper[k][k] > PIVOT_TOL * diag[k]
        inverse[k] = jnp.where(good, 1.0 / jnp.where(good, upper[k][k], 1.0), 0.0)
        for i in range(k + 1, ITERS):
            scale = upper[k][i] * inverse[k]
            for j in range(i, ITERS):
                upper[i][j] = upper[i][j] - scale * upper[k][j]
            right[i] = right[i] - scale * right[k]
    y = [None] * ITERS
    for k in reversed(range(ITERS)):
        value = right[k]
        for j in range(k + 1, ITERS):
            value = value - upper[k][j] * y[j]
        y[k] = value * inverse[k]
    return y


def update_kernel(shift_ref, gram_ref, z_ref, mine_ref, coefs_ref, *refs, step, last, rows, cols):
    low_out, next_out, ux, yx, own, stage = refs[-6:]
    parts = [gram_ref[peer] for peer in range(gram_ref.shape[0])]
    while len(parts) > 1:
        parts = [a + b for a, b in zip(parts[0::2], parts[1::2])] + parts[len(parts) // 2 * 2 :]
    total = parts[0]
    g = {}
    per_part = LANES // cols
    for part in range(total.shape[0]):
        turned = jnp.broadcast_to(total[part : part + 1, :], (LANES, LANES)).T
        for index, (i, j) in enumerate(PAIRS[part * per_part : (part + 1) * per_part]):
            g[i, j] = g[j, i] = turned[index * cols : (index + 1) * cols, :]
    y = weights_of(g)
    for k in range(ITERS):
        yx[k] = y[k]

    def span(row, count=1):
        return slice(row * cols, (row + count) * cols)

    for row in range(rows + 2):
        for slot in range(CELLS + 2):
            value = yx[0] * z_ref[0, slot, span(row), :]
            for k in range(1, ITERS):
                value = value + yx[k] * z_ref[k, slot, span(row), :]
            ux[slot, span(row), :] = value
            if not last and 0 < row <= rows and 0 < slot <= CELLS:
                low_out[slot - 1, span(row - 1), :] = value

    def read_u(slot, row):
        return ux[slot, span(row), :]

    double = 2.0 * shift_ref[step, 0:1, :]
    for row in range(rows):
        image = stencil_rows(
            lambda entry, cell: coefs_ref[1, entry, cell, rows + row : rows + row + 1, :],
            range(len(OFFSETS)), read_u, row + 1,
        )
        for cell in range(CELLS):
            value = mine_ref[cell, span(row), :] - double * image[cell]
            if last:
                own[cell, span(row), :] = value
            else:
                next_out[cell, span(row), :] = value
    if last:
        root = jnp.sqrt(double)
        planes = [root * ux[1 + cell, span(1, rows), :] for cell in range(CELLS)]
        write_natural(low_out, 0, planes, stage, rows, cols)
        write_natural(next_out, None, [own[cell] for cell in range(CELLS)], stage, rows, cols)


def vmem():
    return pl.BlockSpec(memory_space=pltpu.VMEM)


def low_block(steps, rows, cols, width, step):
    return pl.BlockSpec((1, rows, cols, width), lambda i: (step, 0, 0, 0))


def smem():
    return pl.BlockSpec(memory_space=pltpu.SMEM)


def shards(stiffness, mass, shifts, factor):
    rows, cols, width = factor.shape
    steps = shifts.shape[0]
    entries = len(OFFSETS)
    peers = lax.axis_size("rows")
    parity = (lax.axis_index("rows") % 2).astype(jnp.int32).reshape(1)
    block = rows * cols
    ext = 3 * rows
    ext_pad = -(-ext // 8) * 8
    f32 = jnp.float32
    gram_rows = -(-len(PAIRS) * cols // LANES)
    assert block == LANES and width == CELLS * LANES

    within = [(i, i ^ 1) for i in range(peers) if i ^ 1 < peers]
    across = [(i, i + 1) for i in range(1, peers - 1, 2)]
    across = across + [(b, a) for a, b in across]

    def exchange(x):
        return lax.ppermute(x, "rows", within), lax.ppermute(x, "rows", across)

    arrays = [
        pltpu.with_memory_space_constraint(array, pltpu.HBM) for array in (shifts, stiffness, mass, factor)
    ]
    chunked = (CELLS, block, LANES)
    stencils, mine, shift_rows = pl.pallas_call(
        pack_kernel,
        in_specs=[pl.BlockSpec(memory_space=pltpu.HBM)] * 4,
        out_specs=[vmem()] * 3,
        out_shape=[
            jax.ShapeDtypeStruct(shape, f32)
            for shape in ((CELLS, 2 * entries * rows, LANES), chunked, (steps, 8, LANES))
        ],
        scratch_shapes=[pltpu.VMEM((width, LANES), f32), pltpu.VMEM((LANES, width), f32)]
        + [pltpu.SMEM(shifts.shape, f32)]
        + [pltpu.VMEM(array.shape, f32) for array in (stiffness, mass, factor)]
        + [pltpu.SemaphoreType.DMA] * 4,
        compiler_params=params(),
        name="pack",
    )(*arrays)

    z_shape = (ITERS, CELLS + 2, (rows + 2) * cols, LANES)
    coef_shape = (2, entries, CELLS, ext_pad, LANES)
    factor_shapes = (
        (entries, CELLS, ext_pad, LANES),
        (PLANES, ext_pad, LANES),
        (3, CHUNK_PLANES, SUB, LANES),
        (CELLS + 2, block, LANES),
    )
    low_shape = (steps, rows, cols, width)
    low_spec = pl.BlockSpec(memory_space=pl.ANY)
    coefs = None
    lowrank = None
    for step in range(steps):
        first = step == 0
        last = step + 1 == steps
        if first:
            beside = (stencils, *exchange(stencils), mine)
            lead_shape, lead_spec = coef_shape, vmem()
            scratch = []
        else:
            beside = (coefs, mine, u_mine) + (() if lowrank is None else (lowrank,))
            lead_shape, lead_spec = low_shape, low_block(steps, rows, cols, width, step - 1)
            scratch = [pltpu.VMEM((width, LANES), f32)]
        even, odd = exchange(mine)
        lead, *factors = pl.pallas_call(
            functools.partial(side_kernel, step=step, rows=rows, cols=cols),
            grid=(1,),
            in_specs=[smem()] + [vmem()] * (5 if first else 4) + [low_spec] * (len(beside) - (4 if first else 3)),
            out_specs=[lead_spec] + [vmem()] * 4,
            out_shape=[jax.ShapeDtypeStruct(shape, f32) for shape in (lead_shape,) + factor_shapes],
            scratch_shapes=[pltpu.VMEM((CELLS - 1, block, LANES), f32), pltpu.VMEM((block, LANES), f32)] + scratch,
            input_output_aliases={} if first or lowrank is None else {5: 0},
            compiler_params=params(),
            name=f"side{step}",
        )(parity, shift_rows, *beside)
        if first:
            coefs = lead
        else:
            lowrank = lead
        shapes = [z_shape, (peers, gram_rows, LANES)]
        scratch = [
            (ITERS + 1, CELLS, ext * cols, LANES),
            (CELLS + 2, ext * cols, LANES),
            (CELLS - 1, ext * cols, LANES),
            (ext * cols, LANES),
            (gram_rows * LANES, LANES),
        ]
        z, gram = pl.pallas_call(
            functools.partial(krylov_kernel, rows=rows, cols=cols, peers=peers),
            in_specs=[smem()] + [vmem()] * 7,
            out_specs=[vmem() for shape in shapes],
            out_shape=[jax.ShapeDtypeStruct(shape, f32) for shape in shapes],
            scratch_shapes=[pltpu.VMEM(shape, f32) for shape in scratch],
            compiler_params=params(),
            name="krylov",
        )(parity, mine, even, odd, *factors)
        gram = lax.all_to_all(gram, "rows", 0, 0)
        shapes = [low_shape, (rows, cols, width)] if last else [chunked, chunked]
        alias = last and lowrank is not None
        u_mine, mine = pl.pallas_call(
            functools.partial(update_kernel, step=step, last=last, rows=rows, cols=cols),
            grid=(1,),
            in_specs=[vmem()] * 5 + ([low_spec] if alias else []),
            out_specs=[low_block(steps, rows, cols, width, step) if last else vmem(), vmem()],
            out_shape=[jax.ShapeDtypeStruct(shape, f32) for shape in shapes],
            scratch_shapes=[
                pltpu.VMEM((CELLS + 2, (rows + 2) * cols, LANES), f32),
                pltpu.VMEM((ITERS, cols, LANES), f32),
                pltpu.VMEM(chunked, f32),
                pltpu.VMEM((width, LANES), f32),
            ],
            input_output_aliases={5: 0} if alias else {},
            compiler_params=params(),
            name=f"update{step}",
        )(*((shift_rows, gram, z, mine, coefs) + ((lowrank,) if alias else ())))
    return u_mine, mine


def solution(mesh):
    in_specs = (P(None, "rows", None), P(None, "rows", None), P(), P("rows", None, None))
    out_specs = (P(None, "rows", None, None), P("rows", None, None))
    return jax.shard_map(shards, mesh=mesh, in_specs=in_specs, out_specs=out_specs, check_vma=False)
```

```python
import functools

import jax
import jax.numpy as jnp
from jax import lax
from jax.experimental import pallas as pl
from jax.experimental.pallas import tpu as pltpu
from jax.sharding import PartitionSpec as P


ITERS = 4
CELLS = 4
LANES = 128
PIVOT_TOL = 3e-7
OFFSETS = ((-1, -1), (-1, 0), (-1, 1), (0, -1), (0, 0), (0, 1), (1, -1), (1, 0), (1, 1))
OFF_ROW = (0, 1, 2, 6, 7, 8)
PAIRS = [(i, j) for i in range(ITERS + 1) for j in range(i, ITERS + 1)]

SUB = 8
DEPTH = LANES // SUB

E1, E2, G0, G1, G2, C0, C1, A3, L0, L1, L2, R0, R1, R2 = range(14)
PLANES = 14
TE, TINV, TH, TL, TR, TC3, TL0N, TR0N = range(8)
SINGLE = 8 * DEPTH
SA, SC, SB1, SF1, SB2, SF2, S4, SINV = range(8)
CHUNK_PLANES = SINGLE + 8


def roll(x, shift, axis=0):
    return pltpu.roll(x, shift % x.shape[axis], axis)


def params():
    return pltpu.CompilerParams(vmem_limit_bytes=40 * 1024 * 1024)


def to_chunks(natural, stage):
    for tile in range(CELLS):
        stage[tile * LANES : (tile + 1) * LANES, :] = natural[:, tile * LANES : (tile + 1) * LANES].T
    return [
        jnp.concatenate(
            [stage[pl.ds(depth * CELLS + cell, SUB, stride=CELLS * DEPTH), :] for depth in range(DEPTH)], axis=0
        ).T
        for cell in range(CELLS)
    ]


def from_chunks(planes, stage):
    for cell in range(CELLS):
        turned = planes[cell].T
        for depth in range(DEPTH):
            stage[pl.ds(depth * CELLS + cell, SUB, stride=CELLS * DEPTH), :] = turned[
                depth * SUB : (depth + 1) * SUB, :
            ]
    return [stage[tile * LANES : (tile + 1) * LANES, :].T for tile in range(CELLS)]


def split(matrix):
    return [matrix[depth * SUB : (depth + 1) * SUB, :] for depth in range(DEPTH)]


def next_chunk(registers):
    return registers[1:] + [roll(registers[0], -1)]


def previous_chunk(registers):
    return [roll(registers[-1], 1)] + registers[:-1]


def pack_kernel(
    shift_hbm, stiff_hbm, mass_hbm, factor_hbm, field_out, mass_out, shifts_out,
    stage, gather, shift_ref, stiff_ref, mass_ref, factor_ref, shift_sem, stiff_sem, mass_sem, factor_sem,
):
    copies = [
        pltpu.make_async_copy(*operands)
        for operands in (
            (factor_hbm, factor_ref, factor_sem),
            (stiff_hbm, stiff_ref, stiff_sem),
            (mass_hbm, mass_ref, mass_sem),
            (shift_hbm, shift_ref, shift_sem),
        )
    ]
    for copy in copies:
        copy.start()
    rows, cols, width = factor_ref.shape
    entries = len(OFFSETS)
    gather[...] = jnp.zeros(gather.shape, jnp.float32)
    for which, ref in enumerate((stiff_ref, mass_ref)):
        copies[1 + which].wait()
        for entry in range(entries):
            at = (which * entries + entry) * rows
            gather[at : at + rows, :] = ref[entry]
    copies[3].wait()
    for step in range(shifts_out.shape[0]):
        shifts_out[step] = jnp.full(shifts_out.shape[1:], shift_ref[step], jnp.float32)
    planes = to_chunks(gather[...], stage)
    count = entries * rows
    lane = lax.broadcasted_iota(jnp.int32, (count, LANES), 1)
    column = (lax.broadcasted_iota(jnp.int32, (count, LANES), 0) // rows) % 3
    for cell in range(CELLS):
        stiff = planes[cell][0:count, :]
        mass = planes[cell][count : 2 * count, :]
        plane = stiff + shift_ref[0] * mass
        outside = None
        if cell == 0:
            outside = (lane == 0) & (column == 0)
        if cell == CELLS - 1:
            outside = (lane == LANES - 1) & (column == 2)
        if outside is not None:
            plane = jnp.where(outside, 0.0, plane)
            mass = jnp.where(outside, 0.0, mass)
        field_out[cell, rows * cols : rows * cols + count, :] = plane
        mass_out[cell] = mass
    copies[0].wait()
    planes = to_chunks(factor_ref[...].reshape(rows * cols, width), stage)
    for cell in range(CELLS):
        field_out[cell, 0 : rows * cols, :] = planes[cell]


def factor_chunks(group, below, center, above, c3, l0, r0, chunk):
    l0n, r0n = next_chunk(l0), next_chunk(r0)
    center = [center[v] + c3[v] * l0n[v] for v in range(DEPTH)]
    above = [c3[v] * r0n[v] for v in range(DEPTH)]

    def put(index, value):
        chunk[group, index] = value

    for v in range(DEPTH):
        put(TC3 * DEPTH + v, c3[v])
        put(TL0N * DEPTH + v, l0n[v])
        put(TR0N * DEPTH + v, r0n[v])
    last = DEPTH - 1
    inv, hi, left = [], [], []
    for v in range(last):
        if v == 0:
            inv.append(1.0 / center[0])
            left.append(-below[0])
        else:
            e = below[v] * inv[v - 1]
            put(TE * DEPTH + v, e)
            inv.append(1.0 / (center[v] - e * above[v - 1]))
            left.append(-e * left[v - 1])
        hi.append(above[v] * inv[v])
        put(TINV * DEPTH + v, inv[v])
        put(TH * DEPTH + v, hi[v])
    l = [None] * last
    r = [None] * last
    for v in reversed(range(last)):
        l[v] = left[v] * inv[v]
        if v == last - 1:
            r[v] = -hi[v]
        else:
            l[v] = l[v] - hi[v] * l[v + 1]
            r[v] = -hi[v] * r[v + 1]
        put(TL * DEPTH + v, l[v])
        put(TR * DEPTH + v, r[v])
    put(SINGLE + SA, below[last])
    put(SINGLE + SC, above[last])
    b = below[last] * l[last - 1]
    d = center[last] + below[last] * r[last - 1] + above[last] * roll(l[0], -1)
    f = above[last] * roll(r[0], -1)
    slot = SB1
    stride = 1
    while stride < SUB:
        inverse = 1.0 / d
        from_below = -b * roll(inverse, stride)
        from_above = -f * roll(inverse, -stride)
        d = d + from_below * roll(f, stride) + from_above * roll(b, -stride)
        b, f = from_below * roll(b, stride), from_above * roll(f, -stride)
        if 2 * stride == SUB:
            put(SINGLE + S4, from_below + from_above)
        else:
            put(SINGLE + slot, from_below)
            put(SINGLE + slot + 1, from_above)
            slot += 2
        stride *= 2
    put(SINGLE + SINV, 1.0 / d)


def solve_chunks(group, q, p0, chunk):
    def get(index):
        return chunk[group, index]

    p0n = next_chunk(p0)
    q = [q[v] - get(TC3 * DEPTH + v) * p0n[v] for v in range(DEPTH)]
    last = DEPTH - 1
    f = [q[0]]
    for v in range(1, last):
        f.append(q[v] - get(TE * DEPTH + v) * f[v - 1])
    p = [None] * last
    for v in reversed(range(last)):
        p[v] = f[v] * get(TINV * DEPTH + v)
        if v < last - 1:
            p[v] = p[v] - get(TH * DEPTH + v) * p[v + 1]
    s = q[last] - get(SINGLE + SA) * p[last - 1] - get(SINGLE + SC) * roll(p[0], -1)
    s = s + get(SINGLE + SB1) * roll(s, 1) + get(SINGLE + SF1) * roll(s, -1)
    s = s + get(SINGLE + SB2) * roll(s, 2) + get(SINGLE + SF2) * roll(s, -2)
    s = s + get(SINGLE + S4) * roll(s, 4)
    s = s * get(SINGLE + SINV)
    before = roll(s, 1)
    x = [p[v] + get(TL * DEPTH + v) * before + get(TR * DEPTH + v) * s for v in range(last)] + [s]
    xn = next_chunk(x)
    x0n = [p0n[v] + get(TL0N * DEPTH + v) * x[v] + get(TR0N * DEPTH + v) * xn[v] for v in range(DEPTH)]
    return x, previous_chunk(x), x0n


def join_rows(out, own_ref, even_ref, odd_ref, low_is_even, rows, base):
    for entry in range(len(OFFSETS)):
        at = slice(base + entry * rows, base + (entry + 1) * rows)
        for cell in range(CELLS):
            even = even_ref[cell, at, :]
            odd = odd_ref[cell, at, :]
            out[entry, cell, 0:rows, :] = jnp.where(low_is_even, even, odd)
            out[entry, cell, rows : 2 * rows, :] = own_ref[cell, at, :]
            out[entry, cell, 2 * rows : 3 * rows, :] = jnp.where(low_is_even, odd, even)


def build_factors(line, inner, chunk, rows, cols, ext, groups=(0, 1, 2)):
    a = [line[3, cell, 0:ext, :] for cell in range(CELLS)]
    d = [line[4, cell, 0:ext, :] for cell in range(CELLS)]
    c = [line[5, cell, 0:ext, :] for cell in range(CELLS)]
    d = [jnp.where(x <= 0.0, 1.0, x) for x in d]
    g0 = 1.0 / d[0]
    e1 = a[1] * g0
    g1 = 1.0 / (d[1] - e1 * c[0])
    e2 = a[2] * g1
    g2 = 1.0 / (d[2] - e2 * c[1])
    f0 = -a[0]
    f1 = -e1 * f0
    f2 = -e2 * f1
    l2 = f2 * g2
    l1 = (f1 - c[1] * l2) * g1
    l0 = (f0 - c[0] * l1) * g0
    r2 = -c[2] * g2
    r1 = -c[1] * r2 * g1
    r0 = -c[0] * r1 * g0
    for index, value in (
        (E1, e1), (E2, e2), (G0, g0), (G1, g1), (G2, g2), (C0, c[0]), (C1, c[1]), (A3, a[3]),
        (L0, l0), (L1, l1), (L2, l2), (R0, r0), (R1, r1), (R2, r2),
    ):
        inner[index, 0:ext, :] = value
    planes = (a[3] * l2, d[3] + a[3] * r2, c[3], l0, r0)
    for group in groups:
        turned = [
            split(
                jnp.concatenate(
                    [
                        jnp.broadcast_to(plane[row : row + 1, :], (cols, LANES))
                        for row in range(group * rows, (group + 1) * rows)
                    ],
                    axis=0,
                ).T
            )
            for plane in planes
        ]
        below, center, c3, l0t, r0t = turned
        factor_chunks(group, below, center, None, c3, l0t, r0t, chunk)


def stencil_rows(coef, entries, read, row):
    out = []
    for cell in range(CELLS):
        total = None
        for entry in entries:
            offset = OFFSETS[entry]
            term = coef(entry, cell) * read(1 + cell + offset[1], row + offset[0])
            total = term if total is None else total + term
        out.append(total)
    return out


def line_solve(group, wanted, read, inner, chunk, px, qx, zx, base, rows, cols):
    def coef(index, row):
        return inner[index, row : row + 1, :]

    def span(row, count=1):
        return slice((row - base) * cols, (row - base + count) * cols)

    for row in wanted:
        v0, v1, v2, v3 = (read(cell, row) for cell in range(CELLS))
        f1 = v1 - coef(E1, row) * v0
        f2 = v2 - coef(E2, row) * f1
        x2 = f2 * coef(G2, row)
        x1 = (f1 - coef(C1, row) * x2) * coef(G1, row)
        x0 = (v0 - coef(C0, row) * x1) * coef(G0, row)
        px[0, span(row), :] = x0
        px[1, span(row), :] = x1
        px[2, span(row), :] = x2
        qx[span(row), :] = v3 - coef(A3, row) * x2
    at = span(group * rows, rows)
    x, before, after = solve_chunks(group, split(qx[at, :].T), split(px[0, at, :].T), chunk)
    zx[CELLS, at, :] = jnp.concatenate(x, axis=0).T
    zx[0, at, :] = jnp.concatenate(before, axis=0).T
    zx[CELLS + 1, at, :] = jnp.concatenate(after, axis=0).T
    for row in wanted:
        x3 = zx[CELLS, span(row), :]
        x3b = zx[0, span(row), :]
        for cell in range(CELLS - 1):
            zx[1 + cell, span(row), :] = (
                px[cell, span(row), :] + coef(L0 + cell, row) * x3b + coef(R0 + cell, row) * x3
            )


def own_kernel(mine_ref, z_out, line, inner, chunk, px, qx, *, rows, cols):
    line[...] = jnp.zeros(line.shape, jnp.float32)
    for entry in (3, 4, 5):
        at = rows * cols + entry * rows
        for cell in range(CELLS):
            line[entry, cell, rows : 2 * rows, :] = mine_ref[cell, at : at + rows, :]
    build_factors(line, inner, chunk, rows, cols, 3 * rows, (1,))
    solve_own(mine_ref, inner, chunk, px, qx, z_out, rows, cols)


def solve_own(mine_ref, inner, chunk, px, qx, z_out, rows, cols):
    def read(cell, row):
        return mine_ref[cell, (row - rows) * cols : (row - rows + 1) * cols, :]

    line_solve(1, list(range(rows, 2 * rows)), read, inner, chunk, px, qx, z_out, rows, rows, cols)


def side_kernel(parity_ref, shift_ref, mine_ref, *refs, step, rows, cols):
    ext = 3 * rows
    low_is_even = parity_ref[0] == 1
    if step == 0:
        even_ref, odd_ref, line, inner, chunk = refs
        join_rows(line, mine_ref, even_ref, odd_ref, low_is_even, rows, rows * cols)
    else:
        if step == 1:
            base_ref, u_ref, mass_ref, even_ref, odd_ref = refs[:5]
            low_out, line, inner, chunk, z_out, mass_all, px, qx, stage = refs[-9:]
            join_rows(mass_all, mass_ref, even_ref, odd_ref, low_is_even, rows, 0)
        else:
            base_ref, u_ref, mass_all = refs[:3]
            low_out, line, inner, chunk, z_out, px, qx, stage = refs[-8:]
        shift = shift_ref[step, 0:1, :] - shift_ref[0, 0:1, :]
        for entry in range(len(OFFSETS)):
            for cell in range(CELLS):
                line[entry, cell, 0:ext, :] = (
                    base_ref[entry, cell, 0:ext, :] + shift * mass_all[entry, cell, 0:ext, :]
                )
    build_factors(line, inner, chunk, rows, cols, ext)
    if step > 0:
        solve_own(mine_ref, inner, chunk, px, qx, z_out, rows, cols)
        root = jnp.sqrt(2.0 * shift_ref[step - 1, 0:1, :])
        write_natural(low_out, 0, [root * u_ref[cell] for cell in range(CELLS)], stage, rows, cols)


def write_natural(out, lead, planes, stage, rows, cols):
    tiles = from_chunks(planes, stage)
    for tile in range(len(tiles)):
        value = tiles[tile].reshape(rows, cols, LANES)
        if lead is None:
            out[:, :, tile * LANES : (tile + 1) * LANES] = value
        else:
            out[lead, :, :, tile * LANES : (tile + 1) * LANES] = value


def krylov_kernel(
    parity_ref, mine_ref, even_ref, odd_ref, line, inner, chunk, z_mine,
    z_out, gram_out, wx, zx, px, qx, sums, *, rows, cols, peers,
):
    ext = 3 * rows
    block = rows * cols
    parity = parity_ref[0]
    at_even = jnp.where(parity == 0, 2 * rows, 0)
    at_odd = 2 * rows - at_even
    wx[0, :, pl.ds(rows * cols, block), :] = mine_ref[:, 0:block, :]
    wx[0, :, pl.ds(pl.multiple_of(at_even * cols, cols), block), :] = even_ref[:, 0:block, :]
    wx[0, :, pl.ds(pl.multiple_of(at_odd * cols, cols), block), :] = odd_ref[:, 0:block, :]

    def span(row, count=1):
        return slice(row * cols, (row + count) * cols)

    for k in range(ITERS):
        low, high = k, ext - k

        def read_w(cell, row):
            return wx[k, cell, span(row), :]

        for group in range(ext // rows):
            if k == 0 and group == 1:
                zx[:, span(rows, rows), :] = z_mine[...]
                continue
            wanted = [row for row in range(group * rows, (group + 1) * rows) if low <= row < high]
            line_solve(group, wanted, read_w, inner, chunk, px, qx, zx, 0, rows, cols)
        for row in range(rows - 1, 2 * rows + 1):
            z_out[k, :, span(row - rows + 1), :] = zx[:, span(row), :]

        def read_z(slot, row):
            return zx[slot, span(row), :]

        for row in range(low + 1, high - 1):
            image = stencil_rows(lambda entry, cell: line[entry, cell, row : row + 1, :], OFF_ROW, read_z, row)
            for cell in range(CELLS):
                wx[k + 1, cell, span(row), :] = image[cell]

    for tile in range(cols // 8):
        total = [None] * len(PAIRS)
        for row in range(rows, 2 * rows):
            for cell in range(CELLS):
                at = row * cols + tile * 8
                w = [wx[k, cell, at : at + 8, :] for k in range(ITERS + 1)]
                for index, (i, j) in enumerate(PAIRS):
                    term = w[i] * w[j]
                    total[index] = term if total[index] is None else total[index] + term
        for index in range(len(PAIRS)):
            sums[index * cols + tile * 8 : index * cols + tile * 8 + 8, :] = total[index]
    sums[len(PAIRS) * cols :, :] = jnp.zeros((sums.shape[0] - len(PAIRS) * cols, LANES), jnp.float32)
    for part in range(sums.shape[0] // LANES):
        turned = sums[part * LANES : (part + 1) * LANES, :].T
        gram_out[:, part : part + 1, :] = jnp.broadcast_to(
            jnp.sum(turned, axis=0, keepdims=True)[None], (peers, 1, LANES)
        )


def weights_of(g):
    upper = [
        [(g[i, j] + g[i + 1, j + 1]) + (g[i, j + 1] + g[i + 1, j]) for j in range(ITERS)] for i in range(ITERS)
    ]
    diag = [upper[i][i] for i in range(ITERS)]
    right = [g[0, i] + g[0, i + 1] for i in range(ITERS)]
    inverse = [None] * ITERS
    for k in range(ITERS):
        good = upper[k][k] > PIVOT_TOL * diag[k]
        inverse[k] = jnp.where(good, 1.0 / jnp.where(good, upper[k][k], 1.0), 0.0)
        for i in range(k + 1, ITERS):
            scale = upper[k][i] * inverse[k]
            for j in range(i, ITERS):
                upper[i][j] = upper[i][j] - scale * upper[k][j]
            right[i] = right[i] - scale * right[k]
    y = [None] * ITERS
    for k in reversed(range(ITERS)):
        value = right[k]
        for j in range(k + 1, ITERS):
            value = value - upper[k][j] * y[j]
        y[k] = value * inverse[k]
    return y


def update_kernel(shift_ref, gram_ref, z_ref, mine_ref, mass_ref, *refs, step, last, rows, cols):
    low_out, next_out, ux, yx, own, stage = refs[-6:]
    parts = [gram_ref[peer] for peer in range(gram_ref.shape[0])]
    while len(parts) > 1:
        parts = [a + b for a, b in zip(parts[0::2], parts[1::2])] + parts[len(parts) // 2 * 2 :]
    total = parts[0]
    g = {}
    per_part = LANES // cols
    for part in range(total.shape[0]):
        turned = jnp.broadcast_to(total[part : part + 1, :], (LANES, LANES)).T
        for index, (i, j) in enumerate(PAIRS[part * per_part : (part + 1) * per_part]):
            g[i, j] = g[j, i] = turned[index * cols : (index + 1) * cols, :]
    y = weights_of(g)
    for k in range(ITERS):
        yx[k] = y[k]

    def span(row, count=1):
        return slice(row * cols, (row + count) * cols)

    for row in range(rows + 2):
        for slot in range(CELLS + 2):
            value = yx[0] * z_ref[0, slot, span(row), :]
            for k in range(1, ITERS):
                value = value + yx[k] * z_ref[k, slot, span(row), :]
            ux[slot, span(row), :] = value
            if not last and 0 < row <= rows and 0 < slot <= CELLS:
                low_out[slot - 1, span(row - 1), :] = value

    def read_u(slot, row):
        return ux[slot, span(row), :]

    double = 2.0 * shift_ref[step, 0:1, :]
    for row in range(rows):
        image = stencil_rows(
            lambda entry, cell: mass_ref[cell, entry * rows + row : entry * rows + row + 1, :],
            range(len(OFFSETS)), read_u, row + 1,
        )
        for cell in range(CELLS):
            value = mine_ref[cell, span(row), :] - double * image[cell]
            if last:
                own[cell, span(row), :] = value
            else:
                next_out[cell, span(row), :] = value
    if last:
        root = jnp.sqrt(double)
        planes = [root * ux[1 + cell, span(1, rows), :] for cell in range(CELLS)]
        write_natural(low_out, 0, planes, stage, rows, cols)
        write_natural(next_out, None, [own[cell] for cell in range(CELLS)], stage, rows, cols)


def vmem():
    return pl.BlockSpec(memory_space=pltpu.VMEM)


def low_block(rows, cols, width, step):
    return pl.BlockSpec((1, rows, cols, width), lambda i: (step, 0, 0, 0))


def smem():
    return pl.BlockSpec(memory_space=pltpu.SMEM)


def shards(stiffness, mass, shifts, factor):
    rows, cols, width = factor.shape
    steps = shifts.shape[0]
    entries = len(OFFSETS)
    peers = lax.axis_size("rows")
    parity = (lax.axis_index("rows") % 2).astype(jnp.int32).reshape(1)
    block = rows * cols
    ext = 3 * rows
    ext_pad = -(-ext // 8) * 8
    f32 = jnp.float32
    gram_rows = -(-len(PAIRS) * cols // LANES)
    assert block == LANES and width == CELLS * LANES

    within = [(i, i ^ 1) for i in range(peers) if i ^ 1 < peers]
    across = [(i, i + 1) for i in range(1, peers - 1, 2)]
    across = across + [(b, a) for a, b in across]

    def exchange(x):
        return lax.ppermute(x, "rows", within), lax.ppermute(x, "rows", across)

    arrays = [
        pltpu.with_memory_space_constraint(array, pltpu.HBM) for array in (shifts, stiffness, mass, factor)
    ]
    chunked = (CELLS, block, LANES)
    mine, mass_own, shift_rows = pl.pallas_call(
        pack_kernel,
        in_specs=[pl.BlockSpec(memory_space=pltpu.HBM)] * 4,
        out_specs=[vmem()] * 3,
        out_shape=[
            jax.ShapeDtypeStruct(shape, f32)
            for shape in (
                (CELLS, block + entries * rows, LANES),
                (CELLS, entries * rows, LANES),
                (steps, 8, LANES),
            )
        ],
        scratch_shapes=[pltpu.VMEM((width, LANES), f32), pltpu.VMEM((LANES, width), f32)]
        + [pltpu.SMEM(shifts.shape, f32)]
        + [pltpu.VMEM(array.shape, f32) for array in (stiffness, mass, factor)]
        + [pltpu.SemaphoreType.DMA] * 4,
        compiler_params=params(),
        name="pack",
    )(*arrays)

    z_shape = (ITERS, CELLS + 2, (rows + 2) * cols, LANES)
    line_shape = (entries, CELLS, ext_pad, LANES)
    factor_shapes = (
        line_shape,
        (PLANES, ext_pad, LANES),
        (3, CHUNK_PLANES, SUB, LANES),
        (CELLS + 2, block, LANES),
    )
    solver_shapes = ((CELLS - 1, block, LANES), (block, LANES))
    low_shape = (steps, rows, cols, width)
    low_spec = pl.BlockSpec(memory_space=pl.ANY)
    lowrank = None
    for step in range(steps):
        first = step == 0
        last = step + 1 == steps
        even, odd = exchange(mine)
        if first:
            mass_ghosts = exchange(mass_own)
            z_own = pl.pallas_call(
                functools.partial(own_kernel, rows=rows, cols=cols),
                in_specs=[vmem()],
                out_specs=vmem(),
                out_shape=jax.ShapeDtypeStruct(factor_shapes[3], f32),
                scratch_shapes=[pltpu.VMEM(shape, f32) for shape in factor_shapes[:3] + solver_shapes],
                compiler_params=params(),
                name="own0",
            )(mine)
            beside = (even, odd)
        else:
            beside = (base, u_mine) + ((mass_own, *mass_ghosts) if step == 1 else (mass_all,))
        fixed = len(beside)
        shapes = factor_shapes[:3] if first else factor_shapes
        specs = [vmem()] * len(shapes)
        scratch = [] if first else [pltpu.VMEM(shape, f32) for shape in solver_shapes]
        if not first:
            if lowrank is not None:
                beside = beside + (lowrank,)
            shapes = (low_shape,) + shapes + ((line_shape,) if step == 1 else ())
            specs = [low_block(rows, cols, width, step - 1)] + [vmem()] * (len(shapes) - 1)
            scratch = scratch + [pltpu.VMEM((width, LANES), f32)]
        outs = pl.pallas_call(
            functools.partial(side_kernel, step=step, rows=rows, cols=cols),
            grid=(1,),
            in_specs=[smem()] + [vmem()] * (2 + fixed) + [low_spec] * (len(beside) - fixed),
            out_specs=specs,
            out_shape=[jax.ShapeDtypeStruct(shape, f32) for shape in shapes],
            scratch_shapes=scratch,
            input_output_aliases={3 + fixed: 0} if len(beside) > fixed else {},
            compiler_params=params(),
        )(parity, shift_rows, mine, *beside)
        if not first:
            lowrank, *outs = outs
        if step == 1:
            *outs, mass_all = outs
        factors = tuple(outs)
        if first:
            base = factors[0]
            factors = factors + (z_own,)
        shapes = [z_shape, (peers, gram_rows, LANES)]
        scratch = [
            (ITERS + 1, CELLS, ext * cols, LANES),
            (CELLS + 2, ext * cols, LANES),
            (CELLS - 1, ext * cols, LANES),
            (ext * cols, LANES),
            (gram_rows * LANES, LANES),
        ]
        z, gram = pl.pallas_call(
            functools.partial(krylov_kernel, rows=rows, cols=cols, peers=peers),
            in_specs=[smem()] + [vmem()] * 7,
            out_specs=[vmem() for shape in shapes],
            out_shape=[jax.ShapeDtypeStruct(shape, f32) for shape in shapes],
            scratch_shapes=[pltpu.VMEM(shape, f32) for shape in scratch],
            compiler_params=params(),
            name="krylov",
        )(parity, mine, even, odd, *factors)
        gram = lax.all_to_all(gram, "rows", 0, 0)
        shapes = [low_shape, (rows, cols, width)] if last else [chunked, chunked]
        alias = last and lowrank is not None
        u_mine, mine = pl.pallas_call(
            functools.partial(update_kernel, step=step, last=last, rows=rows, cols=cols),
            grid=(1,),
            in_specs=[vmem()] * 5 + ([low_spec] if alias else []),
            out_specs=[low_block(rows, cols, width, step) if last else vmem(), vmem()],
            out_shape=[jax.ShapeDtypeStruct(shape, f32) for shape in shapes],
            scratch_shapes=[
                pltpu.VMEM((CELLS + 2, (rows + 2) * cols, LANES), f32),
                pltpu.VMEM((ITERS, cols, LANES), f32),
                pltpu.VMEM(chunked, f32),
                pltpu.VMEM((width, LANES), f32),
            ],
            input_output_aliases={5: 0} if alias else {},
            compiler_params=params(),
        )(*((shift_rows, gram, z, mine, mass_own) + ((lowrank,) if alias else ())))
    return u_mine, mine


def solution(mesh):
    in_specs = (P(None, "rows", None), P(None, "rows", None), P(), P("rows", None, None))
    out_specs = (P(None, "rows", None, None), P("rows", None, None))
    return jax.shard_map(shards, mesh=mesh, in_specs=in_specs, out_specs=out_specs, check_vma=False)
```

```python
import functools

import jax
import jax.numpy as jnp
from jax import lax
from jax.experimental import pallas as pl
from jax.experimental.pallas import tpu as pltpu
from jax.sharding import PartitionSpec as P


ITERS = 4
CELLS = 4
LANES = 128
PIVOT_TOL = 3e-7
OFFSETS = ((-1, -1), (-1, 0), (-1, 1), (0, -1), (0, 0), (0, 1), (1, -1), (1, 0), (1, 1))
OFF_ROW = (0, 1, 2, 6, 7, 8)
PAIRS = [(i, j) for i in range(ITERS + 1) for j in range(i, ITERS + 1)]

SUB = 8
DEPTH = LANES // SUB

E1, E2, G0, G1, G2, C0, C1, A3, L0, L1, L2, R0, R1, R2 = range(14)
PLANES = 14
TE, TINV, TH, TL, TR, TC3, TL0N, TR0N = range(8)
SINGLE = 8 * DEPTH
SA, SC, SB1, SF1, SB2, SF2, S4, SINV = range(8)
CHUNK_PLANES = SINGLE + 8


def roll(x, shift, axis=0):
    return pltpu.roll(x, shift % x.shape[axis], axis)


def params():
    return pltpu.CompilerParams(vmem_limit_bytes=40 * 1024 * 1024)


def to_chunks(natural, stage):
    for tile in range(CELLS):
        stage[tile * LANES : (tile + 1) * LANES, :] = natural[:, tile * LANES : (tile + 1) * LANES].T
    return [
        jnp.concatenate(
            [stage[pl.ds(depth * CELLS + cell, SUB, stride=CELLS * DEPTH), :] for depth in range(DEPTH)], axis=0
        ).T
        for cell in range(CELLS)
    ]


def from_chunks(planes, stage):
    for cell in range(CELLS):
        turned = planes[cell].T
        for depth in range(DEPTH):
            stage[pl.ds(depth * CELLS + cell, SUB, stride=CELLS * DEPTH), :] = turned[
                depth * SUB : (depth + 1) * SUB, :
            ]
    return [stage[tile * LANES : (tile + 1) * LANES, :].T for tile in range(CELLS)]


def split(matrix):
    return [matrix[depth * SUB : (depth + 1) * SUB, :] for depth in range(DEPTH)]


def next_chunk(registers):
    return registers[1:] + [roll(registers[0], -1)]


def previous_chunk(registers):
    return [roll(registers[-1], 1)] + registers[:-1]


def pack_kernel(
    shift_hbm, stiff_hbm, mass_hbm, factor_hbm, field_out, mass_out, shifts_out,
    stage, gather, shift_ref, stiff_ref, mass_ref, factor_ref, shift_sem, stiff_sem, mass_sem, factor_sem,
):
    copies = [
        pltpu.make_async_copy(*operands)
        for operands in (
            (factor_hbm, factor_ref, factor_sem),
            (stiff_hbm, stiff_ref, stiff_sem),
            (mass_hbm, mass_ref, mass_sem),
            (shift_hbm, shift_ref, shift_sem),
        )
    ]
    for copy in copies:
        copy.start()
    rows, cols, width = factor_ref.shape
    entries = len(OFFSETS)
    gather[...] = jnp.zeros(gather.shape, jnp.float32)
    for which, ref in enumerate((stiff_ref, mass_ref)):
        copies[1 + which].wait()
        for entry in range(entries):
            at = (which * entries + entry) * rows
            gather[at : at + rows, :] = ref[entry]
    copies[3].wait()
    for step in range(shifts_out.shape[0]):
        shifts_out[step] = jnp.full(shifts_out.shape[1:], shift_ref[step], jnp.float32)
    planes = to_chunks(gather[...], stage)
    count = entries * rows
    lane = lax.broadcasted_iota(jnp.int32, (count, LANES), 1)
    column = (lax.broadcasted_iota(jnp.int32, (count, LANES), 0) // rows) % 3
    for cell in range(CELLS):
        stiff = planes[cell][0:count, :]
        mass = planes[cell][count : 2 * count, :]
        plane = stiff + shift_ref[0] * mass
        outside = None
        if cell == 0:
            outside = (lane == 0) & (column == 0)
        if cell == CELLS - 1:
            outside = (lane == LANES - 1) & (column == 2)
        if outside is not None:
            plane = jnp.where(outside, 0.0, plane)
            mass = jnp.where(outside, 0.0, mass)
        field_out[cell, rows * cols : rows * cols + count, :] = plane
        mass_out[cell] = mass
    copies[0].wait()
    planes = to_chunks(factor_ref[...].reshape(rows * cols, width), stage)
    for cell in range(CELLS):
        field_out[cell, 0 : rows * cols, :] = planes[cell]


def factor_chunks(group, below, center, above, c3, l0, r0, chunk):
    l0n, r0n = next_chunk(l0), next_chunk(r0)
    center = [center[v] + c3[v] * l0n[v] for v in range(DEPTH)]
    above = [c3[v] * r0n[v] for v in range(DEPTH)]

    def put(index, value):
        chunk[group, index] = value

    for v in range(DEPTH):
        put(TC3 * DEPTH + v, c3[v])
        put(TL0N * DEPTH + v, l0n[v])
        put(TR0N * DEPTH + v, r0n[v])
    last = DEPTH - 1
    inv, hi, left = [], [], []
    for v in range(last):
        if v == 0:
            inv.append(1.0 / center[0])
            left.append(-below[0])
        else:
            e = below[v] * inv[v - 1]
            put(TE * DEPTH + v, e)
            inv.append(1.0 / (center[v] - e * above[v - 1]))
            left.append(-e * left[v - 1])
        hi.append(above[v] * inv[v])
        put(TINV * DEPTH + v, inv[v])
        put(TH * DEPTH + v, hi[v])
    l = [None] * last
    r = [None] * last
    for v in reversed(range(last)):
        l[v] = left[v] * inv[v]
        if v == last - 1:
            r[v] = -hi[v]
        else:
            l[v] = l[v] - hi[v] * l[v + 1]
            r[v] = -hi[v] * r[v + 1]
        put(TL * DEPTH + v, l[v])
        put(TR * DEPTH + v, r[v])
    put(SINGLE + SA, below[last])
    put(SINGLE + SC, above[last])
    b = below[last] * l[last - 1]
    d = center[last] + below[last] * r[last - 1] + above[last] * roll(l[0], -1)
    f = above[last] * roll(r[0], -1)
    slot = SB1
    stride = 1
    while stride < SUB:
        inverse = 1.0 / d
        from_below = -b * roll(inverse, stride)
        from_above = -f * roll(inverse, -stride)
        d = d + from_below * roll(f, stride) + from_above * roll(b, -stride)
        b, f = from_below * roll(b, stride), from_above * roll(f, -stride)
        if 2 * stride == SUB:
            put(SINGLE + S4, from_below + from_above)
        else:
            put(SINGLE + slot, from_below)
            put(SINGLE + slot + 1, from_above)
            slot += 2
        stride *= 2
    put(SINGLE + SINV, 1.0 / d)


def solve_chunks(group, q, p0, chunk):
    def get(index):
        return chunk[group, index]

    p0n = next_chunk(p0)
    q = [q[v] - get(TC3 * DEPTH + v) * p0n[v] for v in range(DEPTH)]
    last = DEPTH - 1
    f = [q[0]]
    for v in range(1, last):
        f.append(q[v] - get(TE * DEPTH + v) * f[v - 1])
    p = [None] * last
    for v in reversed(range(last)):
        p[v] = f[v] * get(TINV * DEPTH + v)
        if v < last - 1:
            p[v] = p[v] - get(TH * DEPTH + v) * p[v + 1]
    s = q[last] - get(SINGLE + SA) * p[last - 1] - get(SINGLE + SC) * roll(p[0], -1)
    s = s + get(SINGLE + SB1) * roll(s, 1) + get(SINGLE + SF1) * roll(s, -1)
    s = s + get(SINGLE + SB2) * roll(s, 2) + get(SINGLE + SF2) * roll(s, -2)
    s = s + get(SINGLE + S4) * roll(s, 4)
    s = s * get(SINGLE + SINV)
    before = roll(s, 1)
    x = [p[v] + get(TL * DEPTH + v) * before + get(TR * DEPTH + v) * s for v in range(last)] + [s]
    xn = next_chunk(x)
    x0n = [p0n[v] + get(TL0N * DEPTH + v) * x[v] + get(TR0N * DEPTH + v) * xn[v] for v in range(DEPTH)]
    return x, previous_chunk(x), x0n


def join_rows(out, own_ref, even_ref, odd_ref, low_is_even, rows, base):
    for entry in range(len(OFFSETS)):
        at = slice(base + entry * rows, base + (entry + 1) * rows)
        for cell in range(CELLS):
            even = even_ref[cell, at, :]
            odd = odd_ref[cell, at, :]
            out[entry, cell, 0:rows, :] = jnp.where(low_is_even, even, odd)
            out[entry, cell, rows : 2 * rows, :] = own_ref[cell, at, :]
            out[entry, cell, 2 * rows : 3 * rows, :] = jnp.where(low_is_even, odd, even)


def build_factors(line, inner, chunk, rows, cols, ext, groups=(0, 1, 2)):
    a = [line[3, cell, 0:ext, :] for cell in range(CELLS)]
    d = [line[4, cell, 0:ext, :] for cell in range(CELLS)]
    c = [line[5, cell, 0:ext, :] for cell in range(CELLS)]
    d = [jnp.where(x <= 0.0, 1.0, x) for x in d]
    g0 = 1.0 / d[0]
    e1 = a[1] * g0
    g1 = 1.0 / (d[1] - e1 * c[0])
    e2 = a[2] * g1
    g2 = 1.0 / (d[2] - e2 * c[1])
    f0 = -a[0]
    f1 = -e1 * f0
    f2 = -e2 * f1
    l2 = f2 * g2
    l1 = (f1 - c[1] * l2) * g1
    l0 = (f0 - c[0] * l1) * g0
    r2 = -c[2] * g2
    r1 = -c[1] * r2 * g1
    r0 = -c[0] * r1 * g0
    for index, value in (
        (E1, e1), (E2, e2), (G0, g0), (G1, g1), (G2, g2), (C0, c[0]), (C1, c[1]), (A3, a[3]),
        (L0, l0), (L1, l1), (L2, l2), (R0, r0), (R1, r1), (R2, r2),
    ):
        inner[index, 0:ext, :] = value
    planes = (a[3] * l2, d[3] + a[3] * r2, c[3], l0, r0)
    for group in groups:
        turned = [
            split(
                jnp.concatenate(
                    [
                        jnp.broadcast_to(plane[row : row + 1, :], (cols, LANES))
                        for row in range(group * rows, (group + 1) * rows)
                    ],
                    axis=0,
                ).T
            )
            for plane in planes
        ]
        below, center, c3, l0t, r0t = turned
        factor_chunks(group, below, center, None, c3, l0t, r0t, chunk)


def stencil_rows(coef, entries, read, row):
    out = []
    for cell in range(CELLS):
        total = None
        for entry in entries:
            offset = OFFSETS[entry]
            term = coef(entry, cell) * read(1 + cell + offset[1], row + offset[0])
            total = term if total is None else total + term
        out.append(total)
    return out


def line_solve(group, wanted, read, inner, chunk, px, qx, zx, base, rows, cols):
    def coef(index, row):
        return inner[index, row : row + 1, :]

    def span(row, count=1):
        return slice((row - base) * cols, (row - base + count) * cols)

    for row in wanted:
        v0, v1, v2, v3 = (read(cell, row) for cell in range(CELLS))
        f1 = v1 - coef(E1, row) * v0
        f2 = v2 - coef(E2, row) * f1
        x2 = f2 * coef(G2, row)
        x1 = (f1 - coef(C1, row) * x2) * coef(G1, row)
        x0 = (v0 - coef(C0, row) * x1) * coef(G0, row)
        px[0, span(row), :] = x0
        px[1, span(row), :] = x1
        px[2, span(row), :] = x2
        qx[span(row), :] = v3 - coef(A3, row) * x2
    at = span(group * rows, rows)
    x, before, after = solve_chunks(group, split(qx[at, :].T), split(px[0, at, :].T), chunk)
    zx[CELLS, at, :] = jnp.concatenate(x, axis=0).T
    zx[0, at, :] = jnp.concatenate(before, axis=0).T
    zx[CELLS + 1, at, :] = jnp.concatenate(after, axis=0).T
    for row in wanted:
        x3 = zx[CELLS, span(row), :]
        x3b = zx[0, span(row), :]
        for cell in range(CELLS - 1):
            zx[1 + cell, span(row), :] = (
                px[cell, span(row), :] + coef(L0 + cell, row) * x3b + coef(R0 + cell, row) * x3
            )


def own_kernel(mine_ref, z_out, line, inner, chunk, px, qx, *, rows, cols):
    line[...] = jnp.zeros(line.shape, jnp.float32)
    for entry in (3, 4, 5):
        at = rows * cols + entry * rows
        for cell in range(CELLS):
            line[entry, cell, rows : 2 * rows, :] = mine_ref[cell, at : at + rows, :]
    build_factors(line, inner, chunk, rows, cols, 3 * rows, (1,))
    solve_own(mine_ref, inner, chunk, px, qx, z_out, rows, cols)


def solve_own(mine_ref, inner, chunk, px, qx, z_out, rows, cols):
    def read(cell, row):
        return mine_ref[cell, (row - rows) * cols : (row - rows + 1) * cols, :]

    line_solve(1, list(range(rows, 2 * rows)), read, inner, chunk, px, qx, z_out, rows, rows, cols)


def side_kernel(parity_ref, shift_ref, mine_ref, *refs, step, rows, cols):
    ext = 3 * rows
    low_is_even = parity_ref[0] == 1
    if step == 0:
        even_ref, odd_ref, line, inner, chunk = refs
        join_rows(line, mine_ref, even_ref, odd_ref, low_is_even, rows, rows * cols)
    else:
        if step == 1:
            base_ref, u_ref, mass_ref, even_ref, odd_ref = refs[:5]
            low_out, line, inner, chunk, z_out, mass_all, px, qx, stage = refs[-9:]
            join_rows(mass_all, mass_ref, even_ref, odd_ref, low_is_even, rows, 0)
        else:
            base_ref, u_ref, mass_all = refs[:3]
            low_out, line, inner, chunk, z_out, px, qx, stage = refs[-8:]
        shift = shift_ref[step, 0:1, :] - shift_ref[0, 0:1, :]
        for entry in range(len(OFFSETS)):
            for cell in range(CELLS):
                line[entry, cell, 0:ext, :] = (
                    base_ref[entry, cell, 0:ext, :] + shift * mass_all[entry, cell, 0:ext, :]
                )
    build_factors(line, inner, chunk, rows, cols, ext)
    if step > 0:
        solve_own(mine_ref, inner, chunk, px, qx, z_out, rows, cols)
        root = jnp.sqrt(2.0 * shift_ref[step - 1, 0:1, :])
        write_natural(low_out, 0, [root * u_ref[cell] for cell in range(CELLS)], stage, rows, cols)


def write_natural(out, lead, planes, stage, rows, cols):
    tiles = from_chunks(planes, stage)
    for tile in range(len(tiles)):
        value = tiles[tile].reshape(rows, cols, LANES)
        if lead is None:
            out[:, :, tile * LANES : (tile + 1) * LANES] = value
        else:
            out[lead, :, :, tile * LANES : (tile + 1) * LANES] = value


def krylov_kernel(
    parity_ref, mine_ref, even_ref, odd_ref, line, inner, chunk, z_mine,
    z_out, gram_out, wx, px, qx, sums, *, rows, cols, peers,
):
    ext = 3 * rows
    block = rows * cols
    parity = parity_ref[0]
    at_even = jnp.where(parity == 0, 2 * rows, 0)
    at_odd = 2 * rows - at_even
    wx[0, :, pl.ds(pl.multiple_of(at_even * cols, cols), block), :] = even_ref[:, 0:block, :]
    wx[0, :, pl.ds(pl.multiple_of(at_odd * cols, cols), block), :] = odd_ref[:, 0:block, :]

    def span(row, count=1):
        return slice(row * cols, (row + count) * cols)

    for k in range(ITERS):
        low, high = k, ext - k
        zx = z_out.at[k]

        def read_w(cell, row):
            return wx[k, cell, span(row), :]

        for group in range(ext // rows):
            if k == 0 and group == 1:
                zx[:, span(rows, rows), :] = z_mine[...]
                continue
            wanted = [row for row in range(group * rows, (group + 1) * rows) if low <= row < high]
            line_solve(group, wanted, read_w, inner, chunk, px, qx, zx, 0, rows, cols)

        def read_z(slot, row):
            return zx[slot, span(row), :]

        for row in range(low + 1, high - 1):
            image = stencil_rows(lambda entry, cell: line[entry, cell, row : row + 1, :], OFF_ROW, read_z, row)
            for cell in range(CELLS):
                wx[k + 1, cell, span(row), :] = image[cell]

    for tile in range(cols // 8):
        total = [None] * len(PAIRS)
        for row in range(rows, 2 * rows):
            for cell in range(CELLS):
                at = row * cols + tile * 8
                w = [mine_ref[cell, at - block : at - block + 8, :]]
                w = w + [wx[k, cell, at : at + 8, :] for k in range(1, ITERS + 1)]
                for index, (i, j) in enumerate(PAIRS):
                    term = w[i] * w[j]
                    total[index] = term if total[index] is None else total[index] + term
        for index in range(len(PAIRS)):
            sums[index * cols + tile * 8 : index * cols + tile * 8 + 8, :] = total[index]
    sums[len(PAIRS) * cols :, :] = jnp.zeros((sums.shape[0] - len(PAIRS) * cols, LANES), jnp.float32)
    for part in range(sums.shape[0] // LANES):
        turned = sums[part * LANES : (part + 1) * LANES, :].T
        gram_out[:, part : part + 1, :] = jnp.broadcast_to(
            jnp.sum(turned, axis=0, keepdims=True)[None], (peers, 1, LANES)
        )


def weights_of(g):
    upper = [
        [(g[i, j] + g[i + 1, j + 1]) + (g[i, j + 1] + g[i + 1, j]) for j in range(ITERS)] for i in range(ITERS)
    ]
    diag = [upper[i][i] for i in range(ITERS)]
    right = [g[0, i] + g[0, i + 1] for i in range(ITERS)]
    inverse = [None] * ITERS
    for k in range(ITERS):
        good = upper[k][k] > PIVOT_TOL * diag[k]
        inverse[k] = jnp.where(good, 1.0 / jnp.where(good, upper[k][k], 1.0), 0.0)
        for i in range(k + 1, ITERS):
            scale = upper[k][i] * inverse[k]
            for j in range(i, ITERS):
                upper[i][j] = upper[i][j] - scale * upper[k][j]
            right[i] = right[i] - scale * right[k]
    y = [None] * ITERS
    for k in reversed(range(ITERS)):
        value = right[k]
        for j in range(k + 1, ITERS):
            value = value - upper[k][j] * y[j]
        y[k] = value * inverse[k]
    return y


def update_kernel(shift_ref, gram_ref, z_ref, mine_ref, mass_ref, *refs, step, last, rows, cols):
    low_out, next_out, ux, yx, own, stage = refs[-6:]
    parts = [gram_ref[peer] for peer in range(gram_ref.shape[0])]
    while len(parts) > 1:
        parts = [a + b for a, b in zip(parts[0::2], parts[1::2])] + parts[len(parts) // 2 * 2 :]
    total = parts[0]
    g = {}
    per_part = LANES // cols
    for part in range(total.shape[0]):
        turned = jnp.broadcast_to(total[part : part + 1, :], (LANES, LANES)).T
        for index, (i, j) in enumerate(PAIRS[part * per_part : (part + 1) * per_part]):
            g[i, j] = g[j, i] = turned[index * cols : (index + 1) * cols, :]
    y = weights_of(g)
    for k in range(ITERS):
        yx[k] = y[k]

    def span(row, count=1):
        return slice(row * cols, (row + count) * cols)

    for row in range(rows + 2):
        for slot in range(CELLS + 2):
            value = yx[0] * z_ref[0, slot, span(row + rows - 1), :]
            for k in range(1, ITERS):
                value = value + yx[k] * z_ref[k, slot, span(row + rows - 1), :]
            ux[slot, span(row), :] = value
            if not last and 0 < row <= rows and 0 < slot <= CELLS:
                low_out[slot - 1, span(row - 1), :] = value

    def read_u(slot, row):
        return ux[slot, span(row), :]

    double = 2.0 * shift_ref[step, 0:1, :]
    for row in range(rows):
        image = stencil_rows(
            lambda entry, cell: mass_ref[cell, entry * rows + row : entry * rows + row + 1, :],
            range(len(OFFSETS)), read_u, row + 1,
        )
        for cell in range(CELLS):
            value = mine_ref[cell, span(row), :] - double * image[cell]
            if last:
                own[cell, span(row), :] = value
            else:
                next_out[cell, span(row), :] = value
    if last:
        root = jnp.sqrt(double)
        planes = [root * ux[1 + cell, span(1, rows), :] for cell in range(CELLS)]
        write_natural(low_out, 0, planes, stage, rows, cols)
        write_natural(next_out, None, [own[cell] for cell in range(CELLS)], stage, rows, cols)


def vmem():
    return pl.BlockSpec(memory_space=pltpu.VMEM)


def low_block(rows, cols, width, step):
    return pl.BlockSpec((1, rows, cols, width), lambda i: (step, 0, 0, 0))


def smem():
    return pl.BlockSpec(memory_space=pltpu.SMEM)


def shards(stiffness, mass, shifts, factor):
    rows, cols, width = factor.shape
    steps = shifts.shape[0]
    entries = len(OFFSETS)
    peers = lax.axis_size("rows")
    parity = (lax.axis_index("rows") % 2).astype(jnp.int32).reshape(1)
    block = rows * cols
    ext = 3 * rows
    ext_pad = -(-ext // 8) * 8
    f32 = jnp.float32
    gram_rows = -(-len(PAIRS) * cols // LANES)
    assert block == LANES and width == CELLS * LANES

    within = [(i, i ^ 1) for i in range(peers) if i ^ 1 < peers]
    across = [(i, i + 1) for i in range(1, peers - 1, 2)]
    across = across + [(b, a) for a, b in across]

    def exchange(x):
        return lax.ppermute(x, "rows", within), lax.ppermute(x, "rows", across)

    arrays = [
        pltpu.with_memory_space_constraint(array, pltpu.HBM) for array in (shifts, stiffness, mass, factor)
    ]
    chunked = (CELLS, block, LANES)
    mine, mass_own, shift_rows = pl.pallas_call(
        pack_kernel,
        in_specs=[pl.BlockSpec(memory_space=pltpu.HBM)] * 4,
        out_specs=[vmem()] * 3,
        out_shape=[
            jax.ShapeDtypeStruct(shape, f32)
            for shape in (
                (CELLS, block + entries * rows, LANES),
                (CELLS, entries * rows, LANES),
                (steps, 8, LANES),
            )
        ],
        scratch_shapes=[pltpu.VMEM((width, LANES), f32), pltpu.VMEM((LANES, width), f32)]
        + [pltpu.SMEM(shifts.shape, f32)]
        + [pltpu.VMEM(array.shape, f32) for array in (stiffness, mass, factor)]
        + [pltpu.SemaphoreType.DMA] * 4,
        compiler_params=params(),
        name="pack",
    )(*arrays)

    z_shape = (ITERS, CELLS + 2, ext * cols, LANES)
    line_shape = (entries, CELLS, ext_pad, LANES)
    factor_shapes = (
        line_shape,
        (PLANES, ext_pad, LANES),
        (3, CHUNK_PLANES, SUB, LANES),
        (CELLS + 2, block, LANES),
    )
    solver_shapes = ((CELLS - 1, block, LANES), (block, LANES))
    low_shape = (steps, rows, cols, width)
    low_spec = pl.BlockSpec(memory_space=pl.ANY)
    lowrank = None
    for step in range(steps):
        first = step == 0
        last = step + 1 == steps
        even, odd = exchange(mine)
        if first:
            mass_ghosts = exchange(mass_own)
            z_own = pl.pallas_call(
                functools.partial(own_kernel, rows=rows, cols=cols),
                in_specs=[vmem()],
                out_specs=vmem(),
                out_shape=jax.ShapeDtypeStruct(factor_shapes[3], f32),
                scratch_shapes=[pltpu.VMEM(shape, f32) for shape in factor_shapes[:3] + solver_shapes],
                compiler_params=params(),
                name="own0",
            )(mine)
            beside = (even, odd)
        else:
            beside = (base, u_mine) + ((mass_own, *mass_ghosts) if step == 1 else (mass_all,))
        fixed = len(beside)
        shapes = factor_shapes[:3] if first else factor_shapes
        specs = [vmem()] * len(shapes)
        scratch = [] if first else [pltpu.VMEM(shape, f32) for shape in solver_shapes]
        if not first:
            if lowrank is not None:
                beside = beside + (lowrank,)
            shapes = (low_shape,) + shapes + ((line_shape,) if step == 1 else ())
            specs = [low_block(rows, cols, width, step - 1)] + [vmem()] * (len(shapes) - 1)
            scratch = scratch + [pltpu.VMEM((width, LANES), f32)]
        outs = pl.pallas_call(
            functools.partial(side_kernel, step=step, rows=rows, cols=cols),
            grid=(1,),
            in_specs=[smem()] + [vmem()] * (2 + fixed) + [low_spec] * (len(beside) - fixed),
            out_specs=specs,
            out_shape=[jax.ShapeDtypeStruct(shape, f32) for shape in shapes],
            scratch_shapes=scratch,
            input_output_aliases={3 + fixed: 0} if len(beside) > fixed else {},
            compiler_params=params(),
        )(parity, shift_rows, mine, *beside)
        if not first:
            lowrank, *outs = outs
        if step == 1:
            *outs, mass_all = outs
        factors = tuple(outs)
        if first:
            base = factors[0]
            factors = factors + (z_own,)
        shapes = [z_shape, (peers, gram_rows, LANES)]
        scratch = [
            (ITERS + 1, CELLS, ext * cols, LANES),
            (CELLS - 1, ext * cols, LANES),
            (ext * cols, LANES),
            (gram_rows * LANES, LANES),
        ]
        z, gram = pl.pallas_call(
            functools.partial(krylov_kernel, rows=rows, cols=cols, peers=peers),
            in_specs=[smem()] + [vmem()] * 7,
            out_specs=[vmem() for shape in shapes],
            out_shape=[jax.ShapeDtypeStruct(shape, f32) for shape in shapes],
            scratch_shapes=[pltpu.VMEM(shape, f32) for shape in scratch],
            compiler_params=params(),
            name="krylov",
        )(parity, mine, even, odd, *factors)
        gram = lax.all_to_all(gram, "rows", 0, 0)
        shapes = [low_shape, (rows, cols, width)] if last else [chunked, chunked]
        alias = last and lowrank is not None
        u_mine, mine = pl.pallas_call(
            functools.partial(update_kernel, step=step, last=last, rows=rows, cols=cols),
            grid=(1,),
            in_specs=[vmem()] * 5 + ([low_spec] if alias else []),
            out_specs=[low_block(rows, cols, width, step) if last else vmem(), vmem()],
            out_shape=[jax.ShapeDtypeStruct(shape, f32) for shape in shapes],
            scratch_shapes=[
                pltpu.VMEM((CELLS + 2, (rows + 2) * cols, LANES), f32),
                pltpu.VMEM((ITERS, cols, LANES), f32),
                pltpu.VMEM(chunked, f32),
                pltpu.VMEM((width, LANES), f32),
            ],
            input_output_aliases={5: 0} if alias else {},
            compiler_params=params(),
        )(*((shift_rows, gram, z, mine, mass_own) + ((lowrank,) if alias else ())))
    return u_mine, mine


def solution(mesh):
    in_specs = (P(None, "rows", None), P(None, "rows", None), P(), P("rows", None, None))
    out_specs = (P(None, "rows", None, None), P("rows", None, None))
    return jax.shard_map(shards, mesh=mesh, in_specs=in_specs, out_specs=out_specs, check_vma=False)
```
